256 devices in a mesh: tm: 8 (over x_hi, y), rows: 32 (over x_lo, z, core).
Axes of the slice: x: 4 (x_hi: 2, x_lo: 2; x = x_hi * 2 + x_lo), y: 4, z: 8, core: 2. Of those that a mesh axis runs over, the one named last changes fastest.
Arguments:
- record: bfloat16 [2, 65536, 4096], P(None, 'rows', 'tm'), may hold values from -6 to 6
- seed_list: int32 [4], replicated, may hold values from 0 to 65535
- block_offsets: int32 [2], replicated, may hold values from 0 to 1048575
Outputs:
- range_sketch: float32 [65536, 128], P('rows')
- corange_sketch: float32 [2, 256, 4096], P(None, 'rows', 'tm')
- core_sketch: float32 [384, 384], P('rows')
The draws below stay inside these ranges and needn't reach their ends.
Inputs may be any that keep to these rules, and one draw needn't show every extreme that they name: `seed_list`: entries 0, 1, 2, 3 seed the range, co-range, core row and core column test matrices.
All inputs are finite; a program needn't handle non-finite values.
Results may differ from the reference program's by a relative error of at most 0.0041.
Values sent between devices are 32-bit elements; how exact they have to be, the bound alone decides.
A program may use at most 64 MiB of HBM per device.

```python
import math
import jax
import jax.numpy as jnp
from jax import lax

RANGE = 128
CORANGE = 256
CORE = 384
BLOCKS = 2
STATE_ROWS = 65536
BLOCK_COLS = 4096


def place_ends(result, stream_key, low, largest):
    extent = result.shape
    index_at = [jax.random.randint(jax.random.fold_in(stream_key, axis), (), 0, extent[axis]) for axis in range(len(extent))]
    result = result.at[tuple(index_at)].set(low)
    longest = extent.index(max(extent))
    index_at[longest] = (index_at[longest] + 1) % extent[longest]
    return result.at[tuple(index_at)].set(largest)


def steps_of(own_key, shape, shards, smallest, high):
    loudness, own = 1.0, jax.random.fold_in(own_key, 6)
    for position, blocks in shards:
        heights = jnp.exp(jax.random.uniform(jax.random.fold_in(own, position), (blocks,), jnp.float32, smallest / len(shards), high / len(shards)))
        loudness = loudness * jnp.repeat(heights, shape[position] // blocks).reshape([-1 if axis == position else 1 for axis in range(len(shape))])
    return loudness


def centred(key, extent, deviation, reach, pieces=(), held_as=jnp.bfloat16):
    entries = deviation * jax.random.normal(key, extent, jnp.float32)
    if pieces:
        entries = entries * steps_of(key, extent, pieces, -0.22, 0.18)
    return jnp.clip(entries, -reach, reach).astype(held_as)


def setup_inputs(seed: int = 0) -> dict:
    splits = jax.random.split(jax.random.key(seed), 4)
    return {
        "record": centred(splits[0], (BLOCKS, STATE_ROWS, BLOCK_COLS), 1.0, 6.0, ((1, 32), (2, 8))),
        "seed_list": place_ends(jax.random.randint(splits[1], (4,), 0, 65536), jax.random.fold_in(splits[1], 1), 0, 65535).astype(jnp.int32),
        "block_offsets": jax.random.randint(splits[2], (BLOCKS,), 0, 1048576).astype(jnp.int32),
    }


def shift_down(values, amount):
    return lax.shift_right_logical(values, jnp.full(values.shape, amount, jnp.int32))

def sketch_matrix(seed_value, first_ids, second_ids, factor):
    hashed = first_ids[:, None] * 668265263 + second_ids[None, :] * 374761393 + seed_value * 625341585
    hashed = jnp.bitwise_xor(hashed, shift_down(hashed, 15))
    hashed = hashed * 739982445
    hashed = jnp.bitwise_xor(hashed, shift_down(hashed, 12))
    hashed = hashed * 695872825
    hashed = jnp.bitwise_xor(hashed, shift_down(hashed, 15))
    byte_sum = jnp.bitwise_and(hashed, 255)
    byte_sum = byte_sum + jnp.bitwise_and(shift_down(hashed, 8), 255)
    byte_sum = byte_sum + jnp.bitwise_and(shift_down(hashed, 16), 255)
    byte_sum = byte_sum + jnp.bitwise_and(shift_down(hashed, 24), 255)
    return ((byte_sum - 510).astype(jnp.float32) * factor).astype(jnp.bfloat16)

def reference(record, seed_list, block_offsets):
    row_factor = 1.0 / (147.8 * math.sqrt(STATE_ROWS))
    col_factor = 1.0 / (147.8 * math.sqrt(BLOCKS * BLOCK_COLS))
    row_ids = jnp.arange(STATE_ROWS, dtype=jnp.int32)
    psi_rows = sketch_matrix(seed_list[1], jnp.arange(CORANGE, dtype=jnp.int32), row_ids, row_factor)
    phi_rows = sketch_matrix(seed_list[2], jnp.arange(CORE, dtype=jnp.int32), row_ids, row_factor)
    col_base = jnp.arange(BLOCK_COLS, dtype=jnp.int32)
    range_sketch = jnp.zeros((STATE_ROWS, RANGE), jnp.float32)
    core_sketch = jnp.zeros((CORE, CORE), jnp.float32)
    coranges = []
    for number in range(BLOCKS):
        matrix = record[number]
        col_ids = block_offsets[number] + col_base
        omega_cols = sketch_matrix(seed_list[0], col_ids, jnp.arange(RANGE, dtype=jnp.int32), col_factor)
        xi_cols = sketch_matrix(seed_list[3], jnp.arange(CORE, dtype=jnp.int32), col_ids, col_factor)
        range_sketch = range_sketch + jnp.dot(matrix, omega_cols, preferred_element_type=jnp.float32)
        coranges.append(jnp.dot(psi_rows, matrix, preferred_element_type=jnp.float32))
        projected = jnp.dot(phi_rows, matrix, preferred_element_type=jnp.float32)
        core_sketch = core_sketch + jnp.dot(projected, xi_cols.astype(jnp.float32).T, precision=lax.Precision.HIGHEST)
    return (range_sketch, jnp.stack(coranges), core_sketch)
```

```python
import functools
import math

import jax
import jax.numpy as jnp
from jax import lax
from jax.experimental import pallas as pl
from jax.experimental.pallas import tpu as pltpu
from jax.sharding import PartitionSpec as P

RANGE = 128
CORANGE = 256
CORE = 384
C_A = 668265263
C_B = 374761393
C_S = 625341585
MESH = pl.DeviceIdType.MESH

YS = 4
ZS = 8
STREAMS = 2
HALF_PSI = CORANGE // 2
HALF_PHI = CORE // 2
HALF = HALF_PSI + HALF_PHI
KC = 512


def srl(values, amount):
    return lax.shift_right_logical(values, jnp.full(values.shape, amount, jnp.int32))


def gauss(base, factor):
    h = base ^ srl(base, 15)
    h = h * 739982445
    h = h ^ srl(h, 12)
    h = h * 695872825
    h = h ^ srl(h, 15)
    pairs = (h & 0x00FF00FF) + (srl(h, 8) & 0x00FF00FF)
    total = (pairs + srl(pairs, 16)) & 0x7FF
    return ((total - 510).astype(jnp.float32) * factor).astype(jnp.bfloat16)


def wrapped(number):
    return (number + (1 << 31)) % (1 << 32) - (1 << 31)


def iota(shape, dim):
    return lax.broadcasted_iota(jnp.int32, shape, dim)


def kernel(
    row_factor, col_factor, rows_dev, cols_dev,
    seeds, offsets, record,
    range_out, corange_out, core_out,
    rec, omega, xit, ids, lhs0, lhs1, acc_a, acc_b, core_a, core_b,
    part, rb1, rb2, rb3, fwd, ysum, xb,
    got_cor, got_core, zr_cor, zr_core, zs_cor, zs_core, xl_cor, xl_core, tmb,
    in_sem, s1s, s1r, s2s, s2r, s3s, s3r, xs, xr, g1s, g1r, g2s, g2r,
    ds, dr, zs, zr, ls, lr, ts, tr,
):
    tm, rw = lax.axis_index("tm"), lax.axis_index("rows")
    xh, y = tm // YS, lax.rem(tm, YS)
    xl, z, c = rw // (2 * ZS), lax.rem(rw // 2, ZS), lax.rem(rw, 2)

    def device(xh=xh, y=y, xl=xl, z=z, c=c):
        return (xh * YS + y, xl * (2 * ZS) + z * 2 + c)

    y_right, y_left = lax.rem(y + 1, YS), lax.rem(y + YS - 1, YS)
    y_far = lax.rem(y + 2, YS)
    right, left = device(y=y_right), device(y=y_left)
    x_peer = device(xh=1 - xh)
    xl_peer = device(xl=1 - xl)
    partner = device(c=1 - c)
    z_up, z_down = device(z=lax.rem(z + 1, ZS)), device(z=lax.rem(z + ZS - 1, ZS))
    tm_peers = [(lax.rem(tm + i, 2 * YS), rw) for i in range(1, 2 * YS)]

    barrier = pltpu.get_barrier_semaphore()
    greeted = [partner, z_up, z_down, xl_peer, *tm_peers]
    for other in greeted:
        pl.semaphore_signal(barrier, inc=1, device_id=other, device_id_type=MESH)

    chunk = rows_dev // YS
    run = chunk // STREAMS // 2

    def rows_of(d, s, half=None):
        if half is None:
            return pl.ds(pl.multiple_of(d * chunk + s * 2 * run, run), 2 * run)
        return pl.ds(pl.multiple_of(d * chunk + (s * 2 + half) * run, run), run)

    order = [y_far, y_right, y_left, y]
    loads = []
    for i, d in enumerate(order):
        where = pl.ds(pl.multiple_of(d * chunk, chunk), chunk)
        load = pltpu.make_async_copy(record.at[:, where, :], rec.at[:, where, :], in_sem.at[i])
        load.start()
        loads.append(load)

    def send(src, dst, ssem, rsem, to):
        copy = pltpu.make_async_remote_copy(
            src, dst, ssem, rsem, device_id=to, device_id_type=MESH
        )
        copy.start()
        return copy

    sent = []

    lanes = iota((64, 128), 1)
    subs = iota((64, 128), 0)
    pattern_o = subs * C_A + lanes * C_B
    pattern_x = subs * C_B + lanes * C_A
    blocks = 2
    for k in range(blocks):
        col0 = offsets[k] + tm * cols_dev

        def omega_rows(i, _, k=k, col0=col0):
            base = pattern_o + ((col0 + i * 64) * C_A + seeds[0] * C_S)
            omega[pl.ds(pl.multiple_of(k * cols_dev + i * 64, 64), 64), :] = gauss(base, col_factor)
            return 0

        lax.fori_loop(0, cols_dev // 64, omega_rows, 0)

    def range_chunk(d):
        def block(i, _):
            where = pl.ds(pl.multiple_of(d * chunk + i * 256, 256), 256)
            part[where, :] = jnp.dot(
                rec[0, where, :], omega[0:cols_dev, :], preferred_element_type=jnp.float32
            ) + jnp.dot(
                rec[1, where, :], omega[cols_dev : 2 * cols_dev, :], preferred_element_type=jnp.float32
            )
            return 0

        lax.fori_loop(0, chunk // 256, block, 0)

    loads[0].wait()
    range_chunk(y_far)
    pl.semaphore_wait(barrier, len(greeted))
    S1, S2, S3, XC, G1, G2 = {}, {}, {}, {}, {}, {}
    for s in range(STREAMS):
        S1[s, 0] = send(part.at[rows_of(y_far, s, 0)], rb1.at[s, 0], s1s.at[s, 0], s1r.at[s, 0], right)
        S1[s, 1] = send(part.at[rows_of(y_far, s, 1)], rb1.at[s, 1], s1s.at[s, 1], s1r.at[s, 1], left)
    loads[1].wait()
    range_chunk(y_right)
    loads[2].wait()
    range_chunk(y_left)
    for s in range(STREAMS):
        S2[s, 0] = send(part.at[rows_of(y_right, s, 1)], rb2.at[s, 0], s2s.at[s, 0], s2r.at[s, 0], right)
        S2[s, 1] = send(part.at[rows_of(y_left, s, 0)], rb2.at[s, 1], s2s.at[s, 1], s2r.at[s, 1], left)
    loads[3].wait()
    range_chunk(y)

    def range_forward(s):
        S1[s, 0].wait_recv()
        fwd[s, 0] = part[rows_of(y_right, s, 0), :] + rb1[s, 0]
        S3[s, 0] = send(fwd.at[s, 0], rb3.at[s, 0], s3s.at[s, 0], s3r.at[s, 0], right)
        S1[s, 1].wait_recv()
        fwd[s, 1] = part[rows_of(y_left, s, 1), :] + rb1[s, 1]
        S3[s, 1] = send(fwd.at[s, 1], rb3.at[s, 1], s3s.at[s, 1], s3r.at[s, 1], left)

    def range_cross(s):
        S2[s, 0].wait_recv()
        S2[s, 1].wait_recv()
        S3[s, 0].wait_recv()
        S3[s, 1].wait_recv()
        ysum[s, 0:run] = part[rows_of(y, s, 0), :] + rb3[s, 0] + rb2[s, 1]
        ysum[s, run : 2 * run] = part[rows_of(y, s, 1), :] + rb2[s, 0] + rb3[s, 1]
        XC[s] = send(ysum.at[s], xb.at[s], xs.at[s], xr.at[s], x_peer)

    def range_spread(s):
        XC[s].wait_recv()
        own = rows_of(y, s)
        range_out[own, :] = ysum[s] + xb[s]
        G1[s, 0] = send(range_out.at[own], range_out.at[own], g1s.at[s, 0], g1r.at[s, 0], right)
        G1[s, 1] = send(range_out.at[own], range_out.at[own], g1s.at[s, 1], g1r.at[s, 1], left)

    def range_relay(s):
        G1[s, 0].wait_recv()
        a = rows_of(y_left, s, 0)
        G2[s, 0] = send(range_out.at[a], range_out.at[a], g2s.at[s, 0], g2r.at[s, 0], right)
        G1[s, 1].wait_recv()
        b = rows_of(y_right, s, 1)
        G2[s, 1] = send(range_out.at[b], range_out.at[b], g2s.at[s, 1], g2r.at[s, 1], left)

    def range_end(s):
        G2[s, 0].wait_recv()
        G2[s, 1].wait_recv()

    for k in range(blocks):
        col0 = offsets[k] + tm * cols_dev

        def xi_rows(i, _, k=k, col0=col0):
            at = pl.ds(pl.multiple_of(k * cols_dev + i * 64, 64), 64)
            for g in range(CORE // 128):
                base = pattern_x + ((col0 + i * 64) * C_B + seeds[3] * C_S + wrapped(g * 128 * C_A))
                xit[at, g * 128 : (g + 1) * 128] = gauss(base, col_factor)
            return 0

        lax.fori_loop(0, cols_dev // 64, xi_rows, 0)

    row0 = rw * rows_dev

    def row_ids(owner_core):
        m = iota((HALF_PSI, 128), 0)
        at_z, rest = m >> 4, m & 15
        psi_id = (rest >> 3) * 128 + at_z * 16 + owner_core * 8 + (rest & 7)
        ids[0:HALF_PSI, :] = psi_id * C_A + iota((HALF_PSI, 128), 1) * C_B + seeds[1] * C_S
        m = iota((HALF_PHI, 128), 0)
        at_z = (m * 2731) >> 16
        rest = m - at_z * 24
        at_x = jnp.where(rest >= 12, 1, 0)
        phi_id = (at_x * (2 * ZS) + at_z * 2 + owner_core) * 12 + (rest - at_x * 12)
        ids[HALF_PSI:HALF, :] = phi_id * C_A + iota((HALF_PHI, 128), 1) * C_B + seeds[2] * C_S

    def hash_chunk(kc, lhs):
        for g in range(KC // 128):
            shift = (row0 + (kc * KC + g * 128)) * C_B
            for r in range(0, HALF, 64):
                lhs[r : r + 64, g * 128 : (g + 1) * 128] = gauss(ids[r : r + 64, :] + shift, row_factor)

    def dot_chunk(kc, lhs, acc):
        for k in range(blocks):
            for n in range(0, cols_dev, 256):
                got = jnp.dot(
                    lhs[...], rec[k, kc * KC : (kc + 1) * KC, n : n + 256], preferred_element_type=jnp.float32
                )
                at = slice(k * cols_dev + n, k * cols_dev + n + 256)
                if kc == 0:
                    acc[:, at] = got
                else:
                    acc[:, at] += got

    def core_dot(acc, core):
        for r in range(0, HALF_PHI, 64):
            rows = acc[HALF_PSI + r : HALF_PSI + r + 64, :]
            high = rows.astype(jnp.bfloat16)
            low = (rows - high.astype(jnp.float32)).astype(jnp.bfloat16)
            core[r : r + 64, :] = jnp.dot(high, xit[...], preferred_element_type=jnp.float32) + jnp.dot(
                low, xit[...], preferred_element_type=jnp.float32
            )

    n_chunks = rows_dev // KC

    def half(owner_core, acc, core, events):
        row_ids(owner_core)
        hash_chunk(0, lhs0)
        for kc in range(n_chunks):
            if kc + 1 < n_chunks:
                hash_chunk(kc + 1, (lhs0, lhs1)[(kc + 1) % 2])
            dot_chunk(kc, (lhs0, lhs1)[kc % 2], acc)
            for event in events.get(kc, ()):
                event()
        core_dot(acc, core)

    half(1 - c, acc_a, core_a, {})
    D = [
        send(acc_a.at[0:HALF_PSI], got_cor, ds.at[0], dr.at[0], partner),
        send(core_a, got_core, ds.at[1], dr.at[1], partner),
    ]
    for s in range(STREAMS):
        range_forward(s)
    half(c, acc_b, core_b, {1: [functools.partial(range_cross, s) for s in range(STREAMS)]})
    for copy in D:
        copy.wait_recv()

    Z = {}

    def z_step(step, up):
        d = lax.rem(z + (5 - step) if up else z + ZS - 5 + step, ZS)
        way = 0 if up else 1
        cor_at = pl.ds(pl.multiple_of(d * 16, 16), 16)
        core_at = pl.ds(pl.multiple_of(d * 24, 8), 24)
        cor = acc_b[cor_at, :] + got_cor[cor_at, :]
        core = core_b[core_at, :] + got_core[core_at, :]
        to = z_up if up else z_down
        i = step - 1
        half_cols = slice(0, cols_dev) if up else slice(cols_dev, 2 * cols_dev)
        half_rows = slice(0, 16) if up else slice(16, 24)
        if step > 1:
            for copy in Z[step - 1, way]:
                copy.wait_recv()
        zs_cor[way, i] = cor
        zs_core[way, i] = core
        if step == 2:
            zs_cor[way, i, :, half_cols] += zr_cor[way, 0, :, half_cols]
            zs_core[way, i, half_rows, :] += zr_core[way, 0, half_rows, :]
        elif step > 2:
            zs_cor[way, i] += zr_cor[way, i - 1]
            zs_core[way, i] += zr_core[way, i - 1]
        cor_pick = (way, i, slice(None), half_cols) if step == 1 else (way, i)
        core_pick = (way, i, half_rows) if step == 1 else (way, i)
        Z[step, way] = [
            send(zs_cor.at[cor_pick], zr_cor.at[cor_pick], zs.at[way, i, 0], zr.at[way, i, 0], to),
            send(zs_core.at[core_pick], zr_core.at[core_pick], zs.at[way, i, 1], zr.at[way, i, 1], to),
        ]

    z_step(1, True)
    z_step(1, False)
    for s in range(STREAMS):
        range_spread(s)
    z_step(2, True)
    z_step(2, False)
    z_step(3, True)
    z_step(3, False)
    for s in range(STREAMS):
        range_relay(s)
    z_step(4, True)
    z_step(4, False)
    own_cor = pl.ds(pl.multiple_of(z * 16, 16), 16)
    own_core = pl.ds(pl.multiple_of(z * 24, 8), 24)
    acc_b[own_cor, :] += got_cor[own_cor, :]
    core_b[own_core, :] += got_core[own_core, :]
    for way in range(2):
        for copy in Z[4, way]:
            copy.wait_recv()
    core_b[own_core, :] += zr_core[0, 3] + zr_core[1, 3]
    acc_b[own_cor, :] += zr_cor[0, 3] + zr_cor[1, 3]
    L = [
        send(core_b.at[own_core], xl_core, ls.at[1], lr.at[1], xl_peer),
        send(
            acc_b.at[pl.ds(pl.multiple_of(z * 16 + (1 - xl) * 8, 8), 8)], xl_cor, ls.at[0], lr.at[0], xl_peer
        ),
    ]
    L[0].wait_recv()
    both = core_b[own_core, :] + xl_core[...]
    share = jnp.where(xl == 0, both[0:12, :], both[12:24, :])
    tmb[tm, 0:12, :] = share
    tmb[tm, 12:16, :] = jnp.zeros((4, CORE), jnp.float32)
    T = [
        send(tmb.at[tm], tmb.at[tm], ts.at[i], tr.at[i], to) for i, to in enumerate(tm_peers)
    ]
    L[1].wait_recv()
    mine = acc_b[pl.ds(pl.multiple_of(z * 16 + xl * 8, 8), 8), :] + xl_cor[...]
    for k in range(blocks):
        corange_out[k] = mine[:, k * cols_dev : (k + 1) * cols_dev]
    for copy in T:
        copy.wait_recv()
    total = tmb[0, 0:12, :]
    for i in range(1, 2 * YS):
        total = total + tmb[i, 0:12, :]
    core_out[...] = total
    for s in range(STREAMS):
        range_end(s)
    for group in (S1, S2, S3, XC, G1, G2):
        for copy in group.values():
            copy.wait_send()
    for copy in [*D, *L, *T, *[copy for pair in Z.values() for copy in pair]]:
        copy.wait_send()


def shards(record, seed_list, block_offsets):
    blocks, rows_dev, cols_dev = record.shape
    rows_count, time_count = lax.axis_size("rows"), lax.axis_size("tm")
    row_factor = 1.0 / (147.8 * math.sqrt(rows_dev * rows_count))
    col_factor = 1.0 / (147.8 * math.sqrt(blocks * cols_dev * time_count))
    run = rows_dev // YS // STREAMS // 2
    f32, bf16 = jnp.float32, jnp.bfloat16
    vmem, dma = pltpu.VMEM, pltpu.SemaphoreType.DMA
    return pl.pallas_call(
        functools.partial(kernel, row_factor, col_factor, rows_dev, cols_dev),
        out_shape=(
            jax.ShapeDtypeStruct((rows_dev, RANGE), f32),
            jax.ShapeDtypeStruct((blocks, CORANGE // rows_count, cols_dev), f32),
            jax.ShapeDtypeStruct((CORE // rows_count, CORE), f32),
        ),
        in_specs=[
            pl.BlockSpec(memory_space=pltpu.SMEM),
            pl.BlockSpec(memory_space=pltpu.SMEM),
            pl.BlockSpec(memory_space=pl.ANY),
        ],
        out_specs=(pl.BlockSpec(memory_space=pltpu.VMEM),) * 3,
        scratch_shapes=[
            vmem((blocks, rows_dev, cols_dev), bf16),
            vmem((blocks * cols_dev, RANGE), bf16),
            vmem((blocks * cols_dev, CORE), bf16),
            vmem((HALF, 128), jnp.int32),
            vmem((HALF, KC), bf16),
            vmem((HALF, KC), bf16),
            vmem((HALF, blocks * cols_dev), f32),
            vmem((HALF, blocks * cols_dev), f32),
            vmem((HALF_PHI, CORE), f32),
            vmem((HALF_PHI, CORE), f32),
            vmem((rows_dev, RANGE), f32),
            vmem((STREAMS, 2, run, RANGE), f32),
            vmem((STREAMS, 2, run, RANGE), f32),
            vmem((STREAMS, 2, run, RANGE), f32),
            vmem((STREAMS, 2, run, RANGE), f32),
            vmem((STREAMS, 2 * run, RANGE), f32),
            vmem((STREAMS, 2 * run, RANGE), f32),
            vmem((HALF_PSI, blocks * cols_dev), f32),
            vmem((HALF_PHI, CORE), f32),
            vmem((2, 4, 16, blocks * cols_dev), f32),
            vmem((2, 4, 24, CORE), f32),
            vmem((2, 4, 16, blocks * cols_dev), f32),
            vmem((2, 4, 24, CORE), f32),
            vmem((8, blocks * cols_dev), f32),
            vmem((24, CORE), f32),
            vmem((2 * YS, 16, CORE), f32),
            dma((YS,)),
            *[dma((STREAMS, 2))] * 6,
            *[dma((STREAMS,))] * 2,
            *[dma((STREAMS, 2))] * 4,
            *[dma((2,))] * 2,
            *[dma((2, 4, 2))] * 2,
            *[dma((2,))] * 2,
            *[dma((2 * YS - 1,))] * 2,
        ],
        compiler_params=pltpu.CompilerParams(collective_id=0, has_side_effects=True),
        name="three_sketch",
    )(seed_list, block_offsets, record)


def solution(mesh):
    placed = (P(None, "rows", "tm"), P(), P())
    return jax.shard_map(
        shards,
        mesh=mesh,
        in_specs=placed,
        out_specs=(P("rows", None), P(None, "rows", "tm"), P("rows", None)),
        check_vma=False,
    )
```

```python
import functools
import math

import jax
import jax.numpy as jnp
from jax import lax
from jax.experimental import pallas as pl
from jax.experimental.pallas import tpu as pltpu
from jax.sharding import PartitionSpec as P

RANGE = 128
CORANGE = 256
CORE = 384
C_A = 668265263
C_B = 374761393
C_S = 625341585
MESH = pl.DeviceIdType.MESH

YS = 4
ZS = 8
STREAMS = 2
HALF_PSI = CORANGE // 2
HALF_PHI = CORE // 2
KC = 512


def srl(values, amount):
    return lax.shift_right_logical(values, jnp.full(values.shape, amount, jnp.int32))


def gauss(base, factor):
    h = base ^ srl(base, 15)
    h = h * 739982445
    h = h ^ srl(h, 12)
    h = h * 695872825
    h = h ^ srl(h, 15)
    pairs = (h & 0x00FF00FF) + (srl(h, 8) & 0x00FF00FF)
    total = (pairs + srl(pairs, 16)) & 0x7FF
    return ((total - 510).astype(jnp.float32) * factor).astype(jnp.bfloat16)


def wrapped(number):
    return (number + (1 << 31)) % (1 << 32) - (1 << 31)


def iota(shape, dim):
    return lax.broadcasted_iota(jnp.int32, shape, dim)


def kernel(
    row_factor, col_factor, rows_dev, cols_dev,
    seeds, offsets, record,
    range_out, corange_out, core_out,
    rec, omega, xit, ids, lhs0, lhs1, proj, cor, core,
    part, rb1, rb2, rb3, fwd, ysum, xb,
    got_cor, got_core, zr_cor, zr_core, zs_cor, zs_core, xl_cor, xl_core, tmb,
    in_sem, s1s, s1r, s2s, s2r, s3s, s3r, xs, xr, g1s, g1r, g2s, g2r,
    ds, dr, zs, zr, ls, lr, ts, tr,
):
    tm, rw = lax.axis_index("tm"), lax.axis_index("rows")
    xh, y = tm // YS, lax.rem(tm, YS)
    xl, z, c = rw // (2 * ZS), lax.rem(rw // 2, ZS), lax.rem(rw, 2)

    def device(xh=xh, y=y, xl=xl, z=z, c=c):
        return (xh * YS + y, xl * (2 * ZS) + z * 2 + c)

    y_right, y_left = lax.rem(y + 1, YS), lax.rem(y + YS - 1, YS)
    y_far = lax.rem(y + 2, YS)
    right, left = device(y=y_right), device(y=y_left)
    x_peer = device(xh=1 - xh)
    xl_peer = device(xl=1 - xl)
    partner = device(c=1 - c)
    z_up, z_down = device(z=lax.rem(z + 1, ZS)), device(z=lax.rem(z + ZS - 1, ZS))
    tm_peers = [(lax.rem(tm + i, 2 * YS), rw) for i in range(1, 2 * YS)]

    barrier = pltpu.get_barrier_semaphore()
    greeted = [partner, z_up, z_down, xl_peer, *tm_peers]
    for other in greeted:
        pl.semaphore_signal(barrier, inc=1, device_id=other, device_id_type=MESH)

    chunk = rows_dev // YS
    run = chunk // STREAMS // 2

    def rows_of(d, s, half=None):
        if half is None:
            return pl.ds(pl.multiple_of(d * chunk + s * 2 * run, run), 2 * run)
        return pl.ds(pl.multiple_of(d * chunk + (s * 2 + half) * run, run), run)

    order = [y_far, y_right, y_left, y]
    loads = []
    for i, d in enumerate(order):
        where = pl.ds(pl.multiple_of(d * chunk, chunk), chunk)
        load = pltpu.make_async_copy(record.at[:, where, :], rec.at[:, where, :], in_sem.at[i])
        load.start()
        loads.append(load)

    def send(src, dst, ssem, rsem, to):
        copy = pltpu.make_async_remote_copy(
            src, dst, ssem, rsem, device_id=to, device_id_type=MESH
        )
        copy.start()
        return copy

    sent = []

    lanes = iota((64, 128), 1)
    subs = iota((64, 128), 0)
    pattern_o = subs * C_A + lanes * C_B
    pattern_x = subs * C_B + lanes * C_A
    blocks = 2
    row0 = rw * rows_dev
    n_chunks = rows_dev // KC
    lhs = (lhs0, lhs1)

    def omega_hash(k):
        col0 = offsets[k] + tm * cols_dev
        for i in range(0, cols_dev, 64):
            base = pattern_o + ((col0 + i) * C_A + seeds[0] * C_S)
            omega[k * cols_dev + i : k * cols_dev + i + 64, :] = gauss(base, col_factor)

    def xi_hash(k):
        col0 = offsets[k] + tm * cols_dev
        for i in range(0, cols_dev, 64):
            for g in range(0, CORE, 128):
                base = pattern_x + ((col0 + i) * C_B + seeds[3] * C_S + wrapped(g * C_A))
                xit[k * cols_dev + i : k * cols_dev + i + 64, g : g + 128] = gauss(base, col_factor)

    def phi_ids():
        m = iota((CORE, 128), 0)
        mine = jnp.where(m >= HALF_PHI, 1, 0)
        m = m - mine * HALF_PHI
        owner_core = jnp.where(mine == 1, c, 1 - c)
        at_z = (m * 2731) >> 16
        rest = m - at_z * 24
        at_x = jnp.where(rest >= 12, 1, 0)
        row = (at_x * (2 * ZS) + at_z * 2 + owner_core) * 12 + (rest - at_x * 12)
        ids[...] = row * C_A + iota((CORE, 128), 1) * C_B + seeds[2] * C_S

    def psi_ids():
        m = iota((CORANGE, 128), 0)
        mine = m >> 7
        owner_core = jnp.where(mine == 1, c, 1 - c)
        row = ((m & 15) >> 3) * 128 + ((m & 127) >> 4) * 16 + owner_core * 8 + (m & 7)
        ids[0:CORANGE, :] = row * C_A + iota((CORANGE, 128), 1) * C_B + seeds[1] * C_S

    def hash_chunk(kc, rows):
        for g in range(0, KC, 128):
            shift = (row0 + (kc * KC + g)) * C_B
            for r in range(0, rows, 64):
                lhs[kc % 2][r : r + 64, g : g + 128] = gauss(ids[r : r + 64, :] + shift, row_factor)

    def dot_chunk(kc, rows, acc):
        for k in range(blocks):
            for n in range(0, cols_dev, 256):
                got = jnp.dot(
                    lhs[kc % 2][0:rows, :],
                    rec[k, kc * KC : (kc + 1) * KC, n : n + 256],
                    preferred_element_type=jnp.float32,
                )
                at = slice(k * cols_dev + n, k * cols_dev + n + 256)
                acc[:, at] = got if kc == 0 else acc[:, at] + got

    def core_dot(r0, rows):
        part_of = proj[r0 : r0 + rows, :]
        high = part_of.astype(jnp.bfloat16)
        low = (part_of - high.astype(jnp.float32)).astype(jnp.bfloat16)
        core[r0 : r0 + rows, :] = jnp.dot(
            high, xit[...], preferred_element_type=jnp.float32
        ) + jnp.dot(low, xit[...], preferred_element_type=jnp.float32)

    def range_chunk(d):
        where = pl.ds(pl.multiple_of(d * chunk, chunk), chunk)
        part[where, :] = jnp.dot(
            rec[0, where, :], omega[0:cols_dev, :], preferred_element_type=jnp.float32
        ) + jnp.dot(
            rec[1, where, :], omega[cols_dev : 2 * cols_dev, :], preferred_element_type=jnp.float32
        )

    S1, S2, S3, XC, G1, G2, Z, D = {}, {}, {}, {}, {}, {}, {}, {}

    def range_forward(s):
        S1[s, 0].wait_recv()
        fwd[s, 0] = part[rows_of(y_right, s, 0), :] + rb1[s, 0]
        S3[s, 0] = send(fwd.at[s, 0], rb3.at[s, 0], s3s.at[s, 0], s3r.at[s, 0], right)
        S1[s, 1].wait_recv()
        fwd[s, 1] = part[rows_of(y_left, s, 1), :] + rb1[s, 1]
        S3[s, 1] = send(fwd.at[s, 1], rb3.at[s, 1], s3s.at[s, 1], s3r.at[s, 1], left)

    def range_cross(s):
        S2[s, 0].wait_recv()
        S2[s, 1].wait_recv()
        S3[s, 0].wait_recv()
        S3[s, 1].wait_recv()
        ysum[s, 0:run] = part[rows_of(y, s, 0), :] + rb3[s, 0] + rb2[s, 1]
        ysum[s, run : 2 * run] = part[rows_of(y, s, 1), :] + rb2[s, 0] + rb3[s, 1]
        XC[s] = send(ysum.at[s], xb.at[s], xs.at[s], xr.at[s], x_peer)

    def range_spread(s):
        XC[s].wait_recv()
        own = rows_of(y, s)
        range_out[own, :] = ysum[s] + xb[s]
        G1[s, 0] = send(range_out.at[own], range_out.at[own], g1s.at[s, 0], g1r.at[s, 0], right)
        G1[s, 1] = send(range_out.at[own], range_out.at[own], g1s.at[s, 1], g1r.at[s, 1], left)

    def range_relay(s):
        G1[s, 0].wait_recv()
        a = rows_of(y_left, s, 0)
        G2[s, 0] = send(range_out.at[a], range_out.at[a], g2s.at[s, 0], g2r.at[s, 0], right)
        G1[s, 1].wait_recv()
        b = rows_of(y_right, s, 1)
        G2[s, 1] = send(range_out.at[b], range_out.at[b], g2s.at[s, 1], g2r.at[s, 1], left)

    def range_end(s):
        G2[s, 0].wait_recv()
        G2[s, 1].wait_recv()

    def z_step(what, step, up):
        d = lax.rem(z + (5 - step) if up else z + ZS - 5 + step, ZS)
        way = 0 if up else 1
        at = pl.ds(pl.multiple_of(d * (24 if what else 16), 8), 24 if what else 16)
        i = step - 1
        to = z_up if up else z_down
        if what:
            kept, got, sums, arrived = core.at[HALF_PHI:CORE], got_core, zs_core, zr_core
            pick = (slice(0, 16) if up else slice(16, 24), slice(None))
        else:
            kept, got, sums, arrived = cor.at[HALF_PSI:CORANGE], got_cor, zs_cor, zr_cor
            pick = (slice(None), slice(0, cols_dev) if up else slice(cols_dev, 2 * cols_dev))
        if step > 1:
            Z[what, step - 1, way].wait_recv()
        total = kept[at, :] + got[at, :]
        if step > 2:
            total = total + arrived[way, i - 1]
        sums[way, i] = total
        if step == 2:
            sums[(way, i, *pick)] += arrived[(way, 0, *pick)]
        pick = (way, i, *pick) if step == 1 else (way, i)
        Z[what, step, way] = send(
            sums.at[pick], arrived.at[pick], zs.at[way, i, what], zr.at[way, i, what], to
        )

    def pair(what, src, dst):
        D[what] = send(src, dst, ds.at[what], dr.at[what], partner)

    phi_ids()
    hash_chunk(0, CORE)
    for load in loads:
        load.wait()
    for kc in range(n_chunks):
        if kc + 1 < n_chunks:
            hash_chunk(kc + 1, CORE)
        else:
            xi_hash(0)
            xi_hash(1)
        dot_chunk(kc, CORE, proj)
    core_dot(0, HALF_PHI)
    pl.semaphore_wait(barrier, len(greeted))
    pair(1, core.at[0:HALF_PHI], got_core)
    core_dot(HALF_PHI, HALF_PHI)
    omega_hash(0)
    omega_hash(1)

    range_chunk(y_far)
    for s in range(STREAMS):
        S1[s, 0] = send(part.at[rows_of(y_far, s, 0)], rb1.at[s, 0], s1s.at[s, 0], s1r.at[s, 0], right)
        S1[s, 1] = send(part.at[rows_of(y_far, s, 1)], rb1.at[s, 1], s1s.at[s, 1], s1r.at[s, 1], left)
    D[1].wait_recv()
    z_step(1, 1, True)
    z_step(1, 1, False)
    psi_ids()
    hash_chunk(0, CORANGE)
    range_chunk(y_right)
    range_chunk(y_left)
    for s in range(STREAMS):
        S2[s, 0] = send(part.at[rows_of(y_right, s, 1)], rb2.at[s, 0], s2s.at[s, 0], s2r.at[s, 0], right)
        S2[s, 1] = send(part.at[rows_of(y_left, s, 0)], rb2.at[s, 1], s2s.at[s, 1], s2r.at[s, 1], left)
    hash_chunk(1, CORANGE)
    dot_chunk(0, CORANGE, cor)
    range_chunk(y)
    z_step(1, 2, True)
    z_step(1, 2, False)
    hash_chunk(2, CORANGE)
    dot_chunk(1, CORANGE, cor)
    range_forward(0)
    hash_chunk(3, CORANGE)
    dot_chunk(2, CORANGE, cor)
    dot_chunk(3, CORANGE, cor)
    pair(0, cor.at[0:HALF_PSI], got_cor)
    for s in range(1, STREAMS):
        range_forward(s)
    z_step(1, 3, True)
    z_step(1, 3, False)
    D[0].wait_recv()
    z_step(0, 1, True)
    z_step(0, 1, False)
    range_cross(0)
    z_step(1, 4, True)
    z_step(1, 4, False)
    for s in range(1, STREAMS):
        range_cross(s)
    z_step(0, 2, True)
    z_step(0, 2, False)
    own_cor = pl.ds(pl.multiple_of(HALF_PSI + z * 16, 16), 16)
    own_core = pl.ds(pl.multiple_of(HALF_PHI + z * 24, 8), 24)
    core[own_core, :] += got_core[pl.ds(pl.multiple_of(z * 24, 8), 24), :]
    cor[own_cor, :] += got_cor[pl.ds(pl.multiple_of(z * 16, 16), 16), :]
    range_spread(0)
    Z[1, 4, 0].wait_recv()
    Z[1, 4, 1].wait_recv()
    core[own_core, :] += zr_core[0, 3] + zr_core[1, 3]
    L1 = send(core.at[own_core], xl_core, ls.at[1], lr.at[1], xl_peer)
    for s in range(1, STREAMS):
        range_spread(s)
    z_step(0, 3, True)
    z_step(0, 3, False)
    range_relay(0)
    L1.wait_recv()
    both = core[own_core, :] + xl_core[...]
    tmb[tm, 0:12, :] = jnp.where(xl == 0, both[0:12, :], both[12:24, :])
    tmb[tm, 12:16, :] = jnp.zeros((4, CORE), jnp.float32)
    T = [
        send(tmb.at[tm], tmb.at[tm], ts.at[i], tr.at[i], to) for i, to in enumerate(tm_peers)
    ]
    for s in range(1, STREAMS):
        range_relay(s)
    z_step(0, 4, True)
    z_step(0, 4, False)
    Z[0, 4, 0].wait_recv()
    Z[0, 4, 1].wait_recv()
    cor[own_cor, :] += zr_cor[0, 3] + zr_cor[1, 3]
    other = pl.ds(pl.multiple_of(HALF_PSI + z * 16 + (1 - xl) * 8, 8), 8)
    L0 = send(cor.at[other], xl_cor, ls.at[0], lr.at[0], xl_peer)
    for copy in T:
        copy.wait_recv()
    total = tmb[0, 0:12, :]
    for i in range(1, 2 * YS):
        total = total + tmb[i, 0:12, :]
    core_out[...] = total
    for s in range(STREAMS):
        range_end(s)
    L0.wait_recv()
    mine = cor[pl.ds(pl.multiple_of(HALF_PSI + z * 16 + xl * 8, 8), 8), :] + xl_cor[...]
    for k in range(blocks):
        corange_out[k] = mine[:, k * cols_dev : (k + 1) * cols_dev]
    for group in (S1, S2, S3, XC, G1, G2, Z, D):
        for copy in group.values():
            copy.wait_send()
    for copy in [L0, L1, *T]:
        copy.wait_send()


def shards(record, seed_list, block_offsets):
    blocks, rows_dev, cols_dev = record.shape
    rows_count, time_count = lax.axis_size("rows"), lax.axis_size("tm")
    row_factor = 1.0 / (147.8 * math.sqrt(rows_dev * rows_count))
    col_factor = 1.0 / (147.8 * math.sqrt(blocks * cols_dev * time_count))
    run = rows_dev // YS // STREAMS // 2
    f32, bf16 = jnp.float32, jnp.bfloat16
    vmem, dma = pltpu.VMEM, pltpu.SemaphoreType.DMA
    shapes = (
        (rows_dev, RANGE),
        (blocks, CORANGE // rows_count, cols_dev),
        (CORE // rows_count, CORE),
    )
    held = pl.pallas_call(
        functools.partial(kernel, row_factor, col_factor, rows_dev, cols_dev),
        out_shape=tuple(pltpu.VMEM(shape, f32) for shape in shapes),
        in_specs=[
            pl.BlockSpec(memory_space=pltpu.SMEM),
            pl.BlockSpec(memory_space=pltpu.SMEM),
            pl.BlockSpec(memory_space=pl.ANY),
        ],
        out_specs=(pl.BlockSpec(memory_space=pltpu.VMEM),) * 3,
        scratch_shapes=[
            vmem((blocks, rows_dev, cols_dev), bf16),
            vmem((blocks * cols_dev, RANGE), bf16),
            vmem((blocks * cols_dev, CORE), bf16),
            vmem((CORE, 128), jnp.int32),
            vmem((CORE, KC), bf16),
            vmem((CORE, KC), bf16),
            vmem((CORE, blocks * cols_dev), f32),
            vmem((CORANGE, blocks * cols_dev), f32),
            vmem((CORE, CORE), f32),
            vmem((rows_dev, RANGE), f32),
            vmem((STREAMS, 2, run, RANGE), f32),
            vmem((STREAMS, 2, run, RANGE), f32),
            vmem((STREAMS, 2, run, RANGE), f32),
            vmem((STREAMS, 2, run, RANGE), f32),
            vmem((STREAMS, 2 * run, RANGE), f32),
            vmem((STREAMS, 2 * run, RANGE), f32),
            vmem((HALF_PSI, blocks * cols_dev), f32),
            vmem((HALF_PHI, CORE), f32),
            vmem((2, 4, 16, blocks * cols_dev), f32),
            vmem((2, 4, 24, CORE), f32),
            vmem((2, 4, 16, blocks * cols_dev), f32),
            vmem((2, 4, 24, CORE), f32),
            vmem((8, blocks * cols_dev), f32),
            vmem((24, CORE), f32),
            vmem((2 * YS, 16, CORE), f32),
            dma((YS,)),
            *[dma((STREAMS, 2))] * 6,
            *[dma((STREAMS,))] * 2,
            *[dma((STREAMS, 2))] * 4,
            *[dma((2,))] * 2,
            *[dma((2, 4, 2))] * 2,
            *[dma((2,))] * 2,
            *[dma((2 * YS - 1,))] * 2,
        ],
        compiler_params=pltpu.CompilerParams(collective_id=0, has_side_effects=True),
        name="three_sketch",
    )(seed_list, block_offsets, record)
    return held


def solution(mesh):
    placed = (P(None, "rows", "tm"), P(), P())
    return jax.shard_map(
        shards,
        mesh=mesh,
        in_specs=placed,
        out_specs=(P("rows", None), P(None, "rows", "tm"), P("rows", None)),
        check_vma=False,
    )
```

```python
import functools
import math

import jax
import jax.numpy as jnp
from jax import lax
from jax.experimental import pallas as pl
from jax.experimental.pallas import tpu as pltpu
from jax.sharding import PartitionSpec as P

RANGE = 128
CORANGE = 256
CORE = 384
C_A = 668265263
C_B = 374761393
C_S = 625341585
MESH = pl.DeviceIdType.MESH

YS = 4
ZS = 8
STREAMS = 4
HALF_PSI = CORANGE // 2
HALF_PHI = CORE // 2
KC = 512


def srl(values, amount):
    return lax.shift_right_logical(values, jnp.full(values.shape, amount, jnp.int32))


def gauss(base, factor):
    h = base ^ srl(base, 15)
    h = h * 739982445
    h = h ^ srl(h, 12)
    h = h * 695872825
    h = h ^ srl(h, 15)
    pairs = (h & 0x00FF00FF) + (srl(h, 8) & 0x00FF00FF)
    total = (pairs + srl(pairs, 16)) & 0x7FF
    return ((total - 510).astype(jnp.float32) * factor).astype(jnp.bfloat16)


def wrapped(number):
    return (number + (1 << 31)) % (1 << 32) - (1 << 31)


def iota(shape, dim):
    return lax.broadcasted_iota(jnp.int32, shape, dim)


def kernel(
    row_factor, col_factor, rows_dev, cols_dev,
    seeds_in, offsets_in, record,
    range_out, corange_out, core_out,
    seeds, offsets, rec, omega, xit, phi_ids, psi_ids, phi_lhs0, phi_lhs1, psi_lhs, proj, cor, core,
    part, rb0, rb1, rb2, fwd, ysum, xb,
    got_cor, got_core, zr_cor, zr_core, zs_cor, zs_core, xl_cor, shares, xg, yg,
    in_sem, out_sem, s1r, cr, xr, g1r, g2r, dr, zr, lr, tr, ur,
):
    tm, rw = lax.axis_index("tm"), lax.axis_index("rows")
    xh, y = tm // YS, lax.rem(tm, YS)
    xl, z, c = rw // (2 * ZS), lax.rem(rw // 2, ZS), lax.rem(rw, 2)

    def device(xh=xh, y=y, xl=xl, z=z, c=c):
        return (xh * YS + y, xl * (2 * ZS) + z * 2 + c)

    y_right, y_left = lax.rem(y + 1, YS), lax.rem(y + YS - 1, YS)
    y_far = lax.rem(y + 2, YS)
    right, left = device(y=y_right), device(y=y_left)
    x_peer = device(xh=1 - xh)
    xl_peer = device(xl=1 - xl)
    partner = device(c=1 - c)
    z_up, z_down = device(z=lax.rem(z + 1, ZS)), device(z=lax.rem(z + ZS - 1, ZS))
    far = device(y=y_far)
    xx_peer = device(xh=1 - xh, xl=1 - xl)

    scalars = [
        pltpu.make_async_copy(seeds_in, seeds, in_sem.at[YS]),
        pltpu.make_async_copy(offsets_in, offsets, in_sem.at[YS + 1]),
    ]
    for load in scalars:
        load.start()
    chunk = rows_dev // YS
    order = [y_far, y_right, y_left, y]
    loads = []
    for i, d in enumerate(order):
        where = pl.ds(pl.multiple_of(d * chunk, chunk), chunk)
        load = pltpu.make_async_copy(record.at[:, where, :], rec.at[:, where, :], in_sem.at[i])
        load.start()
        loads.append(load)

    barrier = pltpu.get_barrier_semaphore()
    greeted = [partner, z_up, z_down, xl_peer, x_peer, xx_peer, right, left, far]
    for other in greeted:
        pl.semaphore_signal(barrier, inc=1, device_id=other, device_id_type=MESH)

    run = chunk // STREAMS // 2

    def rows_of(d, s, half=None):
        if half is None:
            return pl.ds(pl.multiple_of(d * chunk + s * 2 * run, run), 2 * run)
        return pl.ds(pl.multiple_of(d * chunk + (s * 2 + half) * run, run), run)

    sent = [0, 0, 0]

    def send(group, src, dst, rsem, to):
        sent[group] += math.prod(src.shape) * 4
        copy = pltpu.make_async_remote_copy(
            src, dst, out_sem.at[group], rsem, device_id=to, device_id_type=MESH
        )
        copy.start()
        return copy

    def arrive(like, rsem):
        pltpu.make_async_copy(like, like, rsem).wait()

    lanes = iota((64, 128), 1)
    subs = iota((64, 128), 0)
    pattern_o = subs * C_A + lanes * C_B
    pattern_x = subs * C_B + lanes * C_A
    blocks = 2
    row0 = rw * rows_dev
    n_chunks = rows_dev // KC

    def omega_hash(k):
        col0 = offsets[k] + tm * cols_dev
        for i in range(0, cols_dev, 64):
            base = pattern_o + ((col0 + i) * C_A + seeds[0] * C_S)
            omega[k * cols_dev + i : k * cols_dev + i + 64, :] = gauss(base, col_factor)

    def xi_hash(k):
        col0 = offsets[k] + tm * cols_dev
        for i in range(0, cols_dev, 64):
            for g in range(0, CORE, 128):
                base = pattern_x + ((col0 + i) * C_B + seeds[3] * C_S + wrapped(g * C_A))
                xit[k * cols_dev + i : k * cols_dev + i + 64, g : g + 128] = gauss(base, col_factor)

    def make_ids():
        m = iota((CORE, 128), 0)
        mine = jnp.where(m >= HALF_PHI, 1, 0)
        m = m - mine * HALF_PHI
        owner_core = jnp.where(mine == 1, c, 1 - c)
        at_z = (m * 2731) >> 16
        rest = m - at_z * 24
        at_x = jnp.where(rest >= 12, 1, 0)
        row = (at_x * (2 * ZS) + at_z * 2 + owner_core) * 12 + (rest - at_x * 12)
        phi_ids[...] = row * C_A + iota((CORE, 128), 1) * C_B
        m = iota((CORANGE, 128), 0)
        owner_core = jnp.where(m >= HALF_PSI, c, 1 - c)
        row = ((m & 15) >> 3) * 128 + ((m & 127) >> 4) * 16 + owner_core * 8 + (m & 7)
        psi_ids[...] = row * C_A + iota((CORANGE, 128), 1) * C_B

    def row_hash(kc, ids, lhs, seed):
        for g in range(0, KC, 128):
            shift = (row0 + (kc * KC + g)) * C_B + seed * C_S
            for r in range(0, ids.shape[0], 64):
                lhs[r : r + 64, g : g + 128] = gauss(ids[r : r + 64, :] + shift, row_factor)

    def phi_hash(kc):
        row_hash(kc, phi_ids, (phi_lhs0, phi_lhs1)[kc % 2], seeds[2])

    def psi_hash(kc):
        row_hash(kc, psi_ids, psi_lhs.at[:, kc * KC : (kc + 1) * KC], seeds[1])

    def phi_dot(kc):
        for k in range(blocks):
            for n in range(0, cols_dev, 256):
                got = jnp.dot(
                    (phi_lhs0, phi_lhs1)[kc % 2][...],
                    rec[k, kc * KC : (kc + 1) * KC, n : n + 256],
                    preferred_element_type=jnp.float32,
                )
                at = slice(k * cols_dev + n, k * cols_dev + n + 256)
                proj[:, at] = got if kc == 0 else proj[:, at] + got

    def psi_dot(k):
        for n in range(0, cols_dev, 256):
            cor[:, k * cols_dev + n : k * cols_dev + n + 256] = jnp.dot(
                psi_lhs[...], rec[k, :, n : n + 256], preferred_element_type=jnp.float32
            )

    def core_dot(r0, rows):
        part_of = proj[r0 : r0 + rows, :]
        high = part_of.astype(jnp.bfloat16)
        low = (part_of - high.astype(jnp.float32)).astype(jnp.bfloat16)
        core[r0 : r0 + rows, :] = jnp.dot(
            high, xit[...], preferred_element_type=jnp.float32
        ) + jnp.dot(low, xit[...], preferred_element_type=jnp.float32)

    def range_chunk(d):
        where = pl.ds(pl.multiple_of(d * chunk, chunk), chunk)
        part[where, :] = jnp.dot(
            rec[0, where, :], omega[0:cols_dev, :], preferred_element_type=jnp.float32
        ) + jnp.dot(
            rec[1, where, :], omega[cols_dev : 2 * cols_dev, :], preferred_element_type=jnp.float32
        )

    Z, D = {}, {}

    def range_forward(s):
        arrive(rb1.at[s], s1r.at[s])
        fwd[s, 0] = part[rows_of(y_right, s, 0), :] + rb1[s, 0]
        send(0, fwd.at[s, 0], rb2.at[s, 2], cr.at[s], right)
        fwd[s, 1] = part[rows_of(y_left, s, 1), :] + rb1[s, 1]
        send(0, fwd.at[s, 1], rb2.at[s, 3], cr.at[s], left)

    def range_cross(s):
        if s == 0:
            arrive(rb0, cr.at[0])
            ysum[0] = part[rows_of(y, 0), :] + rb0[0] + (rb0[1] + rb0[2])
        else:
            arrive(rb2.at[s], cr.at[s])
            ysum[s, 0:run] = part[rows_of(y, s, 0), :] + rb2[s, 2] + rb2[s, 1]
            ysum[s, run : 2 * run] = part[rows_of(y, s, 1), :] + rb2[s, 0] + rb2[s, 3]
        send(0, ysum.at[s], xb.at[s], xr.at[s], x_peer)

    def range_spread(s):
        arrive(xb.at[s], xr.at[s])
        own = rows_of(y, s)
        range_out[own, :] = ysum[s] + xb[s]
        last = s == STREAMS - 1
        if last:
            send(0, range_out.at[own], range_out.at[own], g2r.at[0], far)
        sem = g2r.at[0] if last else g1r.at[s]
        send(0, range_out.at[own], range_out.at[own], sem, right)
        send(0, range_out.at[own], range_out.at[own], sem, left)

    def range_relay(s):
        arrive(range_out.at[0 : 4 * run], g1r.at[s])
        a = rows_of(y_left, s, 0)
        send(0, range_out.at[a], range_out.at[a], g2r.at[0], right)
        b = rows_of(y_right, s, 1)
        send(0, range_out.at[b], range_out.at[b], g2r.at[0], left)

    def range_end():
        arrive(range_out.at[0 : (2 * (STREAMS - 1) + 6) * run], g2r.at[0])

    def z_step(what, step, up):
        d = lax.rem(z + (5 - step) if up else z + ZS - 5 + step, ZS)
        way = 0 if up else 1
        at = pl.ds(pl.multiple_of(d * (24 if what else 16), 8), 24 if what else 16)
        i = step - 1
        to = z_up if up else z_down
        if what:
            kept, got, sums, arrived = core.at[HALF_PHI:CORE], got_core, zs_core, zr_core
            pick = (slice(0, 16) if up else slice(16, 24), slice(None))
        else:
            kept, got, sums, arrived = cor.at[HALF_PSI:CORANGE], got_cor, zs_cor, zr_cor
            pick = (slice(None), slice(0, cols_dev) if up else slice(cols_dev, 2 * cols_dev))
        if step == 1:
            rows, cols = pick
            at = pl.ds(pl.multiple_of(d * 24 + rows.start, 8), rows.stop - rows.start) if what else at
            sums[(way, 0, *pick)] = kept[at, cols] + got[at, cols]
        else:
            Z[what, step - 1, way].wait_recv()
            total = kept[at, :] + got[at, :]
            if step > 2:
                total = total + arrived[way, i - 1]
            sums[way, i] = total
            if step == 2:
                sums[(way, i, *pick)] += arrived[(way, 0, *pick)]
        pick = (way, i, *pick) if step == 1 else (way, i)
        sem = zr.at[what, 6 if step == 4 else 3 * way + i]
        Z[what, step, way] = send(1, sums.at[pick], arrived.at[pick], sem, to)

    def pair(what, src, dst):
        D[what] = send(2, src, dst, dr.at[what], partner)

    make_ids()
    for load in scalars:
        load.wait()
    omega_hash(0)
    omega_hash(1)
    xi_hash(0)
    loads[0].wait()
    range_chunk(y_far)
    xi_hash(1)
    pl.semaphore_wait(barrier, len(greeted))
    send(0, part.at[rows_of(y_far, 0)], rb0.at[0], cr.at[0], far)
    for s in range(1, STREAMS):
        send(0, part.at[rows_of(y_far, s, 0)], rb1.at[s, 0], s1r.at[s], right)
        send(0, part.at[rows_of(y_far, s, 1)], rb1.at[s, 1], s1r.at[s], left)
    for load in loads[1:]:
        load.wait()
    phi_hash(0)
    range_chunk(y_right)
    range_chunk(y_left)
    send(0, part.at[rows_of(y_right, 0)], rb0.at[1], cr.at[0], right)
    send(0, part.at[rows_of(y_left, 0)], rb0.at[2], cr.at[0], left)
    for s in range(1, STREAMS):
        send(0, part.at[rows_of(y_right, s, 1)], rb2.at[s, 0], cr.at[s], right)
        send(0, part.at[rows_of(y_left, s, 0)], rb2.at[s, 1], cr.at[s], left)
    phi_hash(1)
    phi_dot(0)
    phi_hash(2)
    phi_dot(1)
    phi_hash(3)
    phi_dot(2)
    psi_hash(0)
    phi_dot(3)
    core_dot(0, HALF_PHI)
    pair(2, core.at[0:HALF_PHI], got_core)
    range_forward(1)
    range_chunk(y)
    psi_hash(1)
    core_dot(HALF_PHI, HALF_PHI)
    psi_hash(2)
    range_forward(2)
    range_forward(3)
    psi_hash(3)
    range_cross(0)
    D[2].wait_recv()
    z_step(1, 1, True)
    z_step(1, 1, False)
    psi_dot(0)
    pair(0, cor.at[0:HALF_PSI, 0:cols_dev], got_cor.at[:, 0:cols_dev])
    psi_dot(1)
    pair(1, cor.at[0:HALF_PSI, cols_dev : 2 * cols_dev], got_cor.at[:, cols_dev : 2 * cols_dev])
    D[0].wait_recv()
    z_step(0, 1, True)
    D[1].wait_recv()
    z_step(0, 1, False)
    z_step(1, 2, True)
    z_step(1, 2, False)
    range_cross(1)
    range_cross(2)
    range_spread(0)
    range_cross(3)
    z_step(0, 2, True)
    z_step(0, 2, False)
    z_step(1, 3, True)
    z_step(1, 3, False)
    own_cor = pl.ds(pl.multiple_of(HALF_PSI + z * 16, 16), 16)
    own_core = pl.ds(pl.multiple_of(HALF_PHI + z * 24, 8), 24)
    core[own_core, :] += got_core[pl.ds(pl.multiple_of(z * 24, 8), 24), :]
    cor[own_cor, :] += got_cor[pl.ds(pl.multiple_of(z * 16, 16), 16), :]
    range_spread(1)
    z_step(0, 3, True)
    z_step(0, 3, False)
    range_relay(0)
    range_spread(2)
    z_step(1, 4, True)
    z_step(1, 4, False)
    range_spread(3)
    z_step(0, 4, True)
    z_step(0, 4, False)
    arrive(zr_core.at[0:2, 3], zr.at[1, 6])
    both = core[own_core, :] + zr_core[0, 3] + zr_core[1, 3]
    pad = jnp.zeros((4, CORE), jnp.float32)
    for i in range(2):
        shares[i, 0:12, :] = both[i * 12 : i * 12 + 12, :]
        shares[i, 12:16, :] = pad
    me_x = xh * 2 + xl
    send(2, shares.at[1 - xl], xg.at[me_x], tr.at[0], xl_peer)
    send(2, shares.at[xl], xg.at[me_x], tr.at[0], x_peer)
    send(2, shares.at[1 - xl], xg.at[me_x], tr.at[0], xx_peer)
    xg[me_x] = shares[xl]
    range_relay(1)
    arrive(xg.at[0:3], tr.at[0])
    yg[y] = (xg[0] + xg[1]) + (xg[2] + xg[3])
    for to in (right, left, far):
        send(2, yg.at[y], yg.at[y], ur.at[0], to)
    arrive(zr_cor.at[0:2, 3], zr.at[0, 6])
    cor[own_cor, :] += zr_cor[0, 3] + zr_cor[1, 3]
    other = pl.ds(pl.multiple_of(HALF_PSI + z * 16 + (1 - xl) * 8, 8), 8)
    send(2, cor.at[other], xl_cor, lr.at[0], xl_peer)
    range_relay(2)
    arrive(xl_cor, lr.at[0])
    mine = cor[pl.ds(pl.multiple_of(HALF_PSI + z * 16 + xl * 8, 8), 8), :] + xl_cor[...]
    for k in range(blocks):
        corange_out[k] = mine[:, k * cols_dev : (k + 1) * cols_dev]
    arrive(yg.at[0:3], ur.at[0])
    total = (yg[0] + yg[1]) + (yg[2] + yg[3])
    core_out[...] = total[0:12, :]
    range_end()
    for group, ref in enumerate((rec, part, rec)):
        rows = sent[group] // (ref.shape[-1] * ref.dtype.itemsize)
        view = ref.at[0, 0:rows] if ref is rec else ref.at[0:rows]
        arrive(view, out_sem.at[group])


def put_out(*refs):
    copies = [pltpu.make_async_copy(refs[i], refs[3 + i], refs[6].at[i]) for i in range(3)]
    for copy in copies:
        copy.start()
    for copy in copies:
        copy.wait()


def shards(record, seed_list, block_offsets):
    blocks, rows_dev, cols_dev = record.shape
    rows_count, time_count = lax.axis_size("rows"), lax.axis_size("tm")
    row_factor = 1.0 / (147.8 * math.sqrt(rows_dev * rows_count))
    col_factor = 1.0 / (147.8 * math.sqrt(blocks * cols_dev * time_count))
    run = rows_dev // YS // STREAMS // 2
    f32, bf16 = jnp.float32, jnp.bfloat16
    vmem, dma = pltpu.VMEM, pltpu.SemaphoreType.DMA
    shapes = (
        (rows_dev, RANGE),
        (blocks, CORANGE // rows_count, cols_dev),
        (CORE // rows_count, CORE),
    )
    held = pl.pallas_call(
        functools.partial(kernel, row_factor, col_factor, rows_dev, cols_dev),
        out_shape=tuple(pltpu.VMEM(shape, f32) for shape in shapes),
        in_specs=[
            pl.BlockSpec(memory_space=pl.ANY),
            pl.BlockSpec(memory_space=pl.ANY),
            pl.BlockSpec(memory_space=pl.ANY),
        ],
        out_specs=(pl.BlockSpec(memory_space=pltpu.VMEM),) * 3,
        scratch_shapes=[
            pltpu.SMEM((4,), jnp.int32),
            pltpu.SMEM((blocks,), jnp.int32),
            vmem((blocks, rows_dev, cols_dev), bf16),
            vmem((blocks * cols_dev, RANGE), bf16),
            vmem((blocks * cols_dev, CORE), bf16),
            vmem((CORE, 128), jnp.int32),
            vmem((CORANGE, 128), jnp.int32),
            vmem((CORE, KC), bf16),
            vmem((CORE, KC), bf16),
            vmem((CORANGE, rows_dev), bf16),
            vmem((CORE, blocks * cols_dev), f32),
            vmem((CORANGE, blocks * cols_dev), f32),
            vmem((CORE, CORE), f32),
            vmem((rows_dev, RANGE), f32),
            vmem((3, 2 * run, RANGE), f32),
            vmem((STREAMS, 2, run, RANGE), f32),
            vmem((STREAMS, 4, run, RANGE), f32),
            vmem((STREAMS, 2, run, RANGE), f32),
            vmem((STREAMS, 2 * run, RANGE), f32),
            vmem((STREAMS, 2 * run, RANGE), f32),
            vmem((HALF_PSI, blocks * cols_dev), f32),
            vmem((HALF_PHI, CORE), f32),
            vmem((2, 4, 16, blocks * cols_dev), f32),
            vmem((2, 4, 24, CORE), f32),
            vmem((2, 4, 16, blocks * cols_dev), f32),
            vmem((2, 4, 24, CORE), f32),
            vmem((8, blocks * cols_dev), f32),
            vmem((2, 16, CORE), f32),
            vmem((4, 16, CORE), f32),
            vmem((YS, 16, CORE), f32),
            dma((YS + 2,)),
            dma((3,)),
            dma((STREAMS,)),
            dma((STREAMS,)),
            dma((STREAMS,)),
            dma((STREAMS - 1,)),
            dma((1,)),
            dma((3,)),
            dma((2, 7)),
            dma((1,)),
            dma((1,)),
            dma((1,)),
        ],
        compiler_params=pltpu.CompilerParams(collective_id=0, has_side_effects=True),
        name="three_sketch",
    )(seed_list, block_offsets, record)
    return pl.pallas_call(
        put_out,
        out_shape=tuple(jax.ShapeDtypeStruct(shape, f32) for shape in shapes),
        in_specs=[pl.BlockSpec(memory_space=pltpu.VMEM)] * 3,
        out_specs=(pl.BlockSpec(memory_space=pl.ANY),) * 3,
        scratch_shapes=[dma((3,))],
        name="put_out",
    )(*[pltpu.with_memory_space_constraint(x, pltpu.VMEM) for x in held])


def solution(mesh):
    placed = (P(None, "rows", "tm"), P(), P())
    return jax.shard_map(
        shards,
        mesh=mesh,
        in_specs=placed,
        out_specs=(P("rows", None), P(None, "rows", "tm"), P("rows", None)),
        check_vma=False,
    )
```

```python
import functools
import math

import jax
import jax.numpy as jnp
from jax import lax
from jax.experimental import pallas as pl
from jax.experimental.pallas import tpu as pltpu
from jax.sharding import PartitionSpec as P

RANGE = 128
CORANGE = 256
CORE = 384
C_A = 668265263
C_B = 374761393
C_S = 625341585
MESH = pl.DeviceIdType.MESH

YS = 4
ZS = 8
STREAMS = 4
HALF_PSI = CORANGE // 2
HALF_PHI = CORE // 2
KC = 512


def srl(values, amount):
    return lax.shift_right_logical(values, jnp.full(values.shape, amount, jnp.int32))


def gauss(base, factor):
    h = base ^ srl(base, 15)
    h = h * 739982445
    h = h ^ srl(h, 12)
    h = h * 695872825
    h = h ^ srl(h, 15)
    pairs = (h & 0x00FF00FF) + (srl(h, 8) & 0x00FF00FF)
    total = srl(pairs * 0x00010001, 16)
    return ((total - 510).astype(jnp.float32) * factor).astype(jnp.bfloat16)


def wrapped(number):
    return (number + (1 << 31)) % (1 << 32) - (1 << 31)


def iota(shape, dim):
    return lax.broadcasted_iota(jnp.int32, shape, dim)


def kernel(
    row_factor, col_factor, rows_dev, cols_dev,
    seeds_in, offsets_in, record,
    range_out, corange_out, core_out,
    seeds, offsets, rec, omega, xit, phi_ids, psi_ids, phi_lhs0, phi_lhs1, psi_lhs, proj, cor, core,
    part, rb0, rb1, rb2, fwd, ysum, xb,
    got_cor, got_core, zr_cor, zr_core, zs_cor, zs_core, zs_own, fin, shares, xg, yg,
    in_sem, out_sem, s1r, cr, xr, g1r, g2r, dr, zr, fr, kr, tr, ur,
):
    tm, rw = lax.axis_index("tm"), lax.axis_index("rows")
    xh, y = tm // YS, lax.rem(tm, YS)
    xl, z, c = rw // (2 * ZS), lax.rem(rw // 2, ZS), lax.rem(rw, 2)

    def device(xh=xh, y=y, xl=xl, z=z, c=c):
        return (xh * YS + y, xl * (2 * ZS) + z * 2 + c)

    y_right, y_left = lax.rem(y + 1, YS), lax.rem(y + YS - 1, YS)
    y_far = lax.rem(y + 2, YS)
    right, left = device(y=y_right), device(y=y_left)
    z_up_x, z_down_x = device(z=lax.rem(z + 1, ZS), xl=1 - xl), device(z=lax.rem(z + ZS - 1, ZS), xl=1 - xl)
    z_up3, z_down3 = device(z=lax.rem(z + 3, ZS)), device(z=lax.rem(z + ZS - 3, ZS))
    x_peer = device(xh=1 - xh)
    xl_peer = device(xl=1 - xl)
    partner = device(c=1 - c)
    z_up, z_down = device(z=lax.rem(z + 1, ZS)), device(z=lax.rem(z + ZS - 1, ZS))
    far = device(y=y_far)
    xx_peer = device(xh=1 - xh, xl=1 - xl)

    scalars = [
        pltpu.make_async_copy(seeds_in, seeds, in_sem.at[YS]),
        pltpu.make_async_copy(offsets_in, offsets, in_sem.at[YS + 1]),
    ]
    for load in scalars:
        load.start()
    chunk = rows_dev // YS
    order = [y_far, y_right, y_left, y]
    loads = []
    for i, d in enumerate(order):
        where = pl.ds(pl.multiple_of(d * chunk, chunk), chunk)
        load = pltpu.make_async_copy(record.at[:, where, :], rec.at[:, where, :], in_sem.at[i])
        load.start()
        loads.append(load)

    barrier = pltpu.get_barrier_semaphore()
    greeted = [partner, z_up, z_down, z_up3, z_down3, z_up_x, z_down_x, xl_peer, x_peer, xx_peer, right, left, far]
    for other in greeted:
        pl.semaphore_signal(barrier, inc=1, device_id=other, device_id_type=MESH)

    run = chunk // STREAMS // 2

    def rows_of(d, s, half=None):
        if half is None:
            return pl.ds(pl.multiple_of(d * chunk + s * 2 * run, run), 2 * run)
        return pl.ds(pl.multiple_of(d * chunk + (s * 2 + half) * run, run), run)

    sent = [0, 0, 0]

    def send(group, src, dst, rsem, to):
        sent[group] += math.prod(src.shape) * 4
        copy = pltpu.make_async_remote_copy(
            src, dst, out_sem.at[group], rsem, device_id=to, device_id_type=MESH
        )
        copy.start()
        return copy

    def arrive(like, rsem):
        pltpu.make_async_copy(like, like, rsem).wait()

    lanes = iota((64, 128), 1)
    subs = iota((64, 128), 0)
    pattern_o = subs * C_A + lanes * C_B
    pattern_x = subs * C_B + lanes * C_A
    blocks = 2
    row0 = rw * rows_dev
    n_chunks = rows_dev // KC

    def together(matrix, vector):
        done = 0
        for i, piece in enumerate(matrix):
            piece()
            until = (i + 1) * len(vector) // len(matrix)
            for other in vector[done:until]:
                other()
            done = until

    def run_all(pieces):
        for piece in pieces:
            piece()

    def omega_hash(k):
        col0 = offsets[k] + tm * cols_dev

        def piece(i):
            base = pattern_o + ((col0 + i) * C_A + seeds[0] * C_S)
            omega[k * cols_dev + i : k * cols_dev + i + 64, :] = gauss(base, col_factor)

        return [functools.partial(piece, i) for i in range(0, cols_dev, 64)]

    def xi_hash(k):
        col0 = offsets[k] + tm * cols_dev

        def piece(i, g):
            base = pattern_x + ((col0 + i) * C_B + seeds[3] * C_S + wrapped(g * C_A))
            xit[k * cols_dev + i : k * cols_dev + i + 64, g : g + 128] = gauss(base, col_factor)

        return [functools.partial(piece, i, g) for i in range(0, cols_dev, 64) for g in range(0, CORE, 128)]

    def make_ids():
        m = iota((CORE, 128), 0)
        mine = jnp.where(m >= HALF_PHI, 1, 0)
        m = m - mine * HALF_PHI
        owner_core = jnp.where(mine == 1, c, 1 - c)
        at_z = (m * 2731) >> 16
        rest = m - at_z * 24
        at_x = jnp.where(rest >= 12, 1, 0)
        row = (at_x * (2 * ZS) + at_z * 2 + owner_core) * 12 + (rest - at_x * 12)
        phi_ids[...] = row * C_A + iota((CORE, 128), 1) * C_B
        m = iota((CORANGE, 128), 0)
        owner_core = jnp.where(m >= HALF_PSI, c, 1 - c)
        row = ((m & 15) >> 3) * 128 + ((m & 127) >> 4) * 16 + owner_core * 8 + (m & 7)
        psi_ids[...] = row * C_A + iota((CORANGE, 128), 1) * C_B

    def row_hash(kc, ids, lhs, seed):
        def piece(g, r):
            shift = (row0 + (kc * KC + g)) * C_B + seed * C_S
            lhs[r : r + 64, g : g + 128] = gauss(ids[r : r + 64, :] + shift, row_factor)

        return [functools.partial(piece, g, r) for g in range(0, KC, 128) for r in range(0, ids.shape[0], 64)]

    def phi_hash(kc):
        return row_hash(kc, phi_ids, (phi_lhs0, phi_lhs1)[kc % 2], seeds[2])

    def psi_hash(kc):
        return row_hash(kc, psi_ids, psi_lhs.at[:, kc * KC : (kc + 1) * KC], seeds[1])

    def phi_dot(kc):
        def piece(k, n):
            got = jnp.dot(
                (phi_lhs0, phi_lhs1)[kc % 2][...],
                rec[k, kc * KC : (kc + 1) * KC, n : n + 256],
                preferred_element_type=jnp.float32,
            )
            at = slice(k * cols_dev + n, k * cols_dev + n + 256)
            proj[:, at] = got if kc == 0 else proj[:, at] + got

        return [functools.partial(piece, k, n) for k in range(blocks) for n in range(0, cols_dev, 256)]

    def psi_dot(k):
        def piece(n):
            cor[:, k * cols_dev + n : k * cols_dev + n + 256] = jnp.dot(
                psi_lhs[...], rec[k, :, n : n + 256], preferred_element_type=jnp.float32
            )

        return [functools.partial(piece, n) for n in range(0, cols_dev, 256)]

    def core_dot(r0):
        def piece():
            part_of = proj[r0 : r0 + HALF_PHI, :]
            high = part_of.astype(jnp.bfloat16)
            low = (part_of - high.astype(jnp.float32)).astype(jnp.bfloat16)
            got = jnp.dot(
                jnp.concatenate([high, low], axis=0), xit[...], preferred_element_type=jnp.float32
            )
            core[r0 : r0 + HALF_PHI, :] = got[0:HALF_PHI] + got[HALF_PHI : 2 * HALF_PHI]

        return [piece]

    def range_dot(d):
        def piece(i):
            where = pl.ds(pl.multiple_of(d * chunk + i, 256), 256)
            part[where, :] = jnp.dot(
                rec[0, where, :], omega[0:cols_dev, :], preferred_element_type=jnp.float32
            ) + jnp.dot(
                rec[1, where, :], omega[cols_dev : 2 * cols_dev, :], preferred_element_type=jnp.float32
            )

        return [functools.partial(piece, i) for i in range(0, chunk, 256)]

    D = {}

    def range_forward(s):
        arrive(rb1.at[s], s1r.at[s])
        fwd[s, 0] = part[rows_of(y_right, s, 0), :] + rb1[s, 0]
        send(0, fwd.at[s, 0], rb2.at[s, 2], cr.at[s], right)
        fwd[s, 1] = part[rows_of(y_left, s, 1), :] + rb1[s, 1]
        send(0, fwd.at[s, 1], rb2.at[s, 3], cr.at[s], left)

    def range_cross(s):
        if s == 0:
            arrive(rb0, cr.at[0])
            ysum[0] = part[rows_of(y, 0), :] + rb0[0] + (rb0[1] + rb0[2])
        else:
            arrive(rb2.at[s], cr.at[s])
            ysum[s, 0:run] = part[rows_of(y, s, 0), :] + rb2[s, 2] + rb2[s, 1]
            ysum[s, run : 2 * run] = part[rows_of(y, s, 1), :] + rb2[s, 0] + rb2[s, 3]
        send(0, ysum.at[s], xb.at[s], xr.at[s], x_peer)

    def range_spread(s):
        arrive(xb.at[s], xr.at[s])
        own = rows_of(y, s)
        range_out[own, :] = ysum[s] + xb[s]
        last = s == STREAMS - 1
        if last:
            send(0, range_out.at[own], range_out.at[own], g2r.at[0], far)
        sem = g2r.at[0] if last else g1r.at[s]
        send(0, range_out.at[own], range_out.at[own], sem, right)
        send(0, range_out.at[own], range_out.at[own], sem, left)

    def range_relay(s):
        arrive(range_out.at[0 : 4 * run], g1r.at[s])
        a = rows_of(y_left, s, 0)
        send(0, range_out.at[a], range_out.at[a], g2r.at[0], right)
        b = rows_of(y_right, s, 1)
        send(0, range_out.at[b], range_out.at[b], g2r.at[0], left)

    def range_end():
        arrive(range_out.at[0 : (2 * (STREAMS - 1) + 6) * run], g2r.at[0])

    def cor_of(d, b, row, rows):
        cols = slice(b * cols_dev, (b + 1) * cols_dev)
        at = pl.ds(pl.multiple_of(d * 16 + row, 8), rows)
        mine = pl.ds(pl.multiple_of(HALF_PSI + d * 16 + row, 8), rows)
        return cor[mine, cols] + got_cor[at, cols]

    def cor_step(b, up, step):
        way = 0 if up else 1
        total = cor_of(lax.rem(z + (5 - step) if up else z + ZS - 5 + step, ZS), b, 0, 16)
        if step > (1 if b == way else 2):
            arrive(zr_cor.at[b, way, step - 2], zr.at[b, way, step - 2])
            total = total + zr_cor[b, way, step - 2]
        zs_cor[b, way, step - 1] = total
        if step < 4:
            send(
                1, zs_cor.at[b, way, step - 1], zr_cor.at[b, way, step - 1], zr.at[b, way, step - 1],
                z_up if up else z_down,
            )
        else:
            for other, to in ((0, z_up if up else z_down), (1, z_up_x if up else z_down_x)):
                row = xl * 8 if other == 0 else (1 - xl) * 8
                rows = pl.ds(pl.multiple_of(row, 8), 8)
                send(1, zs_cor.at[b, way, 3, rows], fin.at[b, 2 * way + other], fr.at[b], to)

    def cor_other(b):
        zs_own[b] = cor_of(z, b, (1 - xl) * 8, 8)
        send(1, zs_own.at[b], fin.at[b, 4], fr.at[b], xl_peer)

    def cor_final(b):
        arrive(fin.at[b], fr.at[b])
        corange_out[b] = (
            cor_of(z, b, xl * 8, 8) + fin[b, 4] + (fin[b, 0] + fin[b, 1]) + (fin[b, 2] + fin[b, 3])
        )

    def core_own(d):
        at = pl.ds(pl.multiple_of(d * 24, 8), 24)
        mine = pl.ds(pl.multiple_of(HALF_PHI + d * 24, 8), 24)
        return core[mine, :] + got_core[at, :]

    def core_gather(up):
        way = 0 if up else 1
        rows = slice(0, 16) if up else slice(16, 24)
        to = z_up if up else z_down
        zs_core[way, 0] = core_own(lax.rem(z + 4, ZS))
        zs_core[way, 1] = core_own(lax.rem(z + (2 if up else ZS - 2), ZS))
        send(1, zs_core.at[way, 0, rows], zr_core.at[way, 0, rows], kr.at[way], to)
        send(1, zs_core.at[way, 1], zr_core.at[way, 1], kr.at[way], to)

    def core_deliver(up):
        way = 0 if up else 1
        rows = slice(0, 16) if up else slice(16, 24)
        arrive(core.at[0 : 40 if up else 32], kr.at[way])
        zs_core[way, 2] = core_own(lax.rem(z + (3 if up else ZS - 3), ZS))
        zs_core[way, 2, rows, :] += zr_core[way, 0, rows, :]
        zs_core[way, 3] = core_own(lax.rem(z + (1 if up else ZS - 1), ZS)) + zr_core[way, 1]
        send(1, zs_core.at[way, 2], zr_core.at[way, 2], kr.at[2], z_up3 if up else z_down3)
        send(1, zs_core.at[way, 3], zr_core.at[way, 3], kr.at[2], z_up if up else z_down)

    def pair(what, src, dst):
        D[what] = send(2, src, dst, dr.at[what], partner)

    make_ids()
    for load in scalars:
        load.wait()
    xi = xi_hash(0) + xi_hash(1)
    run_all(omega_hash(0) + omega_hash(1) + xi[0:2])
    loads[0].wait()
    together(range_dot(y_far), xi[2:16])
    pl.semaphore_wait(barrier, len(greeted))
    send(0, part.at[rows_of(y_far, 0)], rb0.at[0], cr.at[0], far)
    for s in range(1, STREAMS):
        send(0, part.at[rows_of(y_far, s, 0)], rb1.at[s, 0], s1r.at[s], right)
        send(0, part.at[rows_of(y_far, s, 1)], rb1.at[s, 1], s1r.at[s], left)
    for load in loads[1:]:
        load.wait()
    together(range_dot(y_right) + range_dot(y_left), xi[16:] + phi_hash(0))
    send(0, part.at[rows_of(y_right, 0)], rb0.at[1], cr.at[0], right)
    send(0, part.at[rows_of(y_left, 0)], rb0.at[2], cr.at[0], left)
    for s in range(1, STREAMS):
        send(0, part.at[rows_of(y_right, s, 1)], rb2.at[s, 0], cr.at[s], right)
        send(0, part.at[rows_of(y_left, s, 0)], rb2.at[s, 1], cr.at[s], left)
    run_all(phi_hash(1) + phi_dot(0) + phi_hash(2) + phi_dot(1) + phi_hash(3) + phi_dot(2) + psi_hash(0)[0:8] + phi_dot(3) + psi_hash(0)[8:] + core_dot(0))
    pair(2, core.at[0:HALF_PHI], got_core)
    run_all(psi_hash(1) + core_dot(HALF_PHI))
    range_forward(1)
    run_all(psi_hash(2) + range_dot(y) + psi_hash(3))
    D[2].wait_recv()
    core_gather(True)
    core_gather(False)
    range_forward(2)
    range_forward(3)
    run_all(psi_dot(0))
    pair(0, cor.at[0:HALF_PSI, 0:cols_dev], got_cor.at[:, 0:cols_dev])
    run_all(psi_dot(1))
    pair(1, cor.at[0:HALF_PSI, cols_dev : 2 * cols_dev], got_cor.at[:, cols_dev : 2 * cols_dev])
    range_cross(0)
    D[0].wait_recv()
    cor_step(0, True, 1)
    cor_step(0, False, 2)
    cor_other(0)
    range_cross(1)
    D[1].wait_recv()
    cor_step(1, True, 2)
    cor_step(1, False, 1)
    cor_other(1)
    range_cross(2)
    core_deliver(True)
    core_deliver(False)
    range_cross(3)
    range_spread(0)
    for b, up, step in ((0, True, 2), (0, False, 3), (1, False, 2), (1, True, 3)):
        cor_step(b, up, step)
    range_spread(1)
    arrive(zr_core.at[0:2, 2:4], kr.at[2])
    both = core_own(z) + (zr_core[0, 2] + zr_core[0, 3]) + (zr_core[1, 2] + zr_core[1, 3])
    pad = jnp.zeros((4, CORE), jnp.float32)
    for i in range(2):
        shares[i, 0:12, :] = both[i * 12 : i * 12 + 12, :]
        shares[i, 12:16, :] = pad
    me_x = xh * 2 + xl
    send(2, shares.at[1 - xl], xg.at[me_x], tr.at[0], xl_peer)
    send(2, shares.at[xl], xg.at[me_x], tr.at[0], x_peer)
    send(2, shares.at[1 - xl], xg.at[me_x], tr.at[0], xx_peer)
    xg[me_x] = shares[xl]
    range_spread(2)
    for b, up, step in ((0, True, 3), (0, False, 4), (1, False, 3), (1, True, 4)):
        cor_step(b, up, step)
    range_relay(0)
    range_spread(3)
    arrive(xg.at[0:3], tr.at[0])
    yg[y] = (xg[0] + xg[1]) + (xg[2] + xg[3])
    for to in (right, left, far):
        send(2, yg.at[y], yg.at[y], ur.at[0], to)
    range_relay(1)
    cor_step(0, True, 4)
    cor_step(1, False, 4)
    range_relay(2)
    arrive(yg.at[0:3], ur.at[0])
    total = (yg[0] + yg[1]) + (yg[2] + yg[3])
    core_out[...] = total[0:12, :]
    cor_final(0)
    cor_final(1)
    range_end()
    for group, ref in enumerate((rec, part, rec)):
        rows = sent[group] // (ref.shape[-1] * ref.dtype.itemsize)
        view = ref.at[0, 0:rows] if ref is rec else ref.at[0:rows]
        arrive(view, out_sem.at[group])


def put_out(*refs):
    copies = [pltpu.make_async_copy(refs[i], refs[3 + i], refs[6].at[i]) for i in range(3)]
    for copy in copies:
        copy.start()
    for copy in copies:
        copy.wait()


def shards(record, seed_list, block_offsets):
    blocks, rows_dev, cols_dev = record.shape
    rows_count, time_count = lax.axis_size("rows"), lax.axis_size("tm")
    row_factor = 1.0 / (147.8 * math.sqrt(rows_dev * rows_count))
    col_factor = 1.0 / (147.8 * math.sqrt(blocks * cols_dev * time_count))
    run = rows_dev // YS // STREAMS // 2
    f32, bf16 = jnp.float32, jnp.bfloat16
    vmem, dma = pltpu.VMEM, pltpu.SemaphoreType.DMA
    shapes = (
        (rows_dev, RANGE),
        (blocks, CORANGE // rows_count, cols_dev),
        (CORE // rows_count, CORE),
    )
    held = pl.pallas_call(
        functools.partial(kernel, row_factor, col_factor, rows_dev, cols_dev),
        out_shape=tuple(pltpu.VMEM(shape, f32) for shape in shapes),
        in_specs=[
            pl.BlockSpec(memory_space=pl.ANY),
            pl.BlockSpec(memory_space=pl.ANY),
            pl.BlockSpec(memory_space=pl.ANY),
        ],
        out_specs=(pl.BlockSpec(memory_space=pltpu.VMEM),) * 3,
        scratch_shapes=[
            pltpu.SMEM((4,), jnp.int32),
            pltpu.SMEM((blocks,), jnp.int32),
            vmem((blocks, rows_dev, cols_dev), bf16),
            vmem((blocks * cols_dev, RANGE), bf16),
            vmem((blocks * cols_dev, CORE), bf16),
            vmem((CORE, 128), jnp.int32),
            vmem((CORANGE, 128), jnp.int32),
            vmem((CORE, KC), bf16),
            vmem((CORE, KC), bf16),
            vmem((CORANGE, rows_dev), bf16),
            vmem((CORE, blocks * cols_dev), f32),
            vmem((CORANGE, blocks * cols_dev), f32),
            vmem((CORE, CORE), f32),
            vmem((rows_dev, RANGE), f32),
            vmem((3, 2 * run, RANGE), f32),
            vmem((STREAMS, 2, run, RANGE), f32),
            vmem((STREAMS, 4, run, RANGE), f32),
            vmem((STREAMS, 2, run, RANGE), f32),
            vmem((STREAMS, 2 * run, RANGE), f32),
            vmem((STREAMS, 2 * run, RANGE), f32),
            vmem((HALF_PSI, blocks * cols_dev), f32),
            vmem((HALF_PHI, CORE), f32),
            vmem((blocks, 2, 3, 16, cols_dev), f32),
            vmem((2, 4, 24, CORE), f32),
            vmem((blocks, 2, 4, 16, cols_dev), f32),
            vmem((2, 4, 24, CORE), f32),
            vmem((blocks, 8, cols_dev), f32),
            vmem((blocks, 5, 8, cols_dev), f32),
            vmem((2, 16, CORE), f32),
            vmem((4, 16, CORE), f32),
            vmem((YS, 16, CORE), f32),
            dma((YS + 2,)),
            dma((3,)),
            dma((STREAMS,)),
            dma((STREAMS,)),
            dma((STREAMS,)),
            dma((STREAMS - 1,)),
            dma((1,)),
            dma((3,)),
            dma((blocks, 2, 3)),
            dma((blocks,)),
            dma((3,)),
            dma((1,)),
            dma((1,)),
        ],
        compiler_params=pltpu.CompilerParams(collective_id=0, has_side_effects=True),
        name="three_sketch",
    )(seed_list, block_offsets, record)
    return pl.pallas_call(
        put_out,
        out_shape=tuple(jax.ShapeDtypeStruct(shape, f32) for shape in shapes),
        in_specs=[pl.BlockSpec(memory_space=pltpu.VMEM)] * 3,
        out_specs=(pl.BlockSpec(memory_space=pl.ANY),) * 3,
        scratch_shapes=[dma((3,))],
        name="put_out",
    )(*[pltpu.with_memory_space_constraint(x, pltpu.VMEM) for x in held])


def solution(mesh):
    placed = (P(None, "rows", "tm"), P(), P())
    return jax.shard_map(
        shards,
        mesh=mesh,
        in_specs=placed,
        out_specs=(P("rows", None), P(None, "rows", "tm"), P("rows", None)),
        check_vma=False,
    )
```

```python
import functools
import math

import jax
import jax.numpy as jnp
from jax import lax
from jax.experimental import pallas as pl
from jax.experimental.pallas import tpu as pltpu
from jax.sharding import PartitionSpec as P

RANGE = 128
CORANGE = 256
CORE = 384
C_A = 668265263
C_B = 374761393
C_S = 625341585
MESH = pl.DeviceIdType.MESH

YS = 4
ZS = 8
STREAMS = 4
HALF_PSI = CORANGE // 2
HALF_PHI = CORE // 2
KC = 512


def srl(values, amount):
    return lax.shift_right_logical(values, jnp.full(values.shape, amount, jnp.int32))


def gauss(base, factor):
    h = base ^ srl(base, 15)
    h = h * 739982445
    h = h ^ srl(h, 12)
    h = h * 695872825
    h = h ^ srl(h, 15)
    pairs = (h & 0x00FF00FF) + (srl(h, 8) & 0x00FF00FF)
    total = srl(pairs * 0x00010001, 16)
    return ((total - 510).astype(jnp.float32) * factor).astype(jnp.bfloat16)


def wrapped(number):
    return (number + (1 << 31)) % (1 << 32) - (1 << 31)


def iota(shape, dim):
    return lax.broadcasted_iota(jnp.int32, shape, dim)


def kernel(
    row_factor, col_factor, rows_dev, cols_dev,
    seeds_in, offsets_in, record,
    range_out, corange_out, core_out,
    seeds, offsets, rec, omega, xit, phi_ids, psi_ids, phi_lhs0, phi_lhs1, psi_lhs, proj, cor, core,
    part, rb0, rb1, rb2, fwd, ysum, xb,
    got_cor, got_core, zr_cor, zr_core, zs_cor, zs_core, zs_own, fin, shares, xg, yg,
    in_sem, out_sem, s1r, cr, xr, g1r, g2r, dr, zr, fr, kr, tr, ur,
):
    tm, rw = lax.axis_index("tm"), lax.axis_index("rows")
    xh, y = tm // YS, lax.rem(tm, YS)
    xl, z, c = rw // (2 * ZS), lax.rem(rw // 2, ZS), lax.rem(rw, 2)

    def device(xh=xh, y=y, xl=xl, z=z, c=c):
        return (xh * YS + y, xl * (2 * ZS) + z * 2 + c)

    y_right, y_left = lax.rem(y + 1, YS), lax.rem(y + YS - 1, YS)
    y_far = lax.rem(y + 2, YS)
    right, left = device(y=y_right), device(y=y_left)
    z_up_x, z_down_x = device(z=lax.rem(z + 1, ZS), xl=1 - xl), device(z=lax.rem(z + ZS - 1, ZS), xl=1 - xl)
    z_up3, z_down3 = device(z=lax.rem(z + 3, ZS)), device(z=lax.rem(z + ZS - 3, ZS))
    x_peer = device(xh=1 - xh)
    xl_peer = device(xl=1 - xl)
    partner = device(c=1 - c)
    z_up, z_down = device(z=lax.rem(z + 1, ZS)), device(z=lax.rem(z + ZS - 1, ZS))
    far = device(y=y_far)
    xx_peer = device(xh=1 - xh, xl=1 - xl)

    barrier = pltpu.get_barrier_semaphore()
    greeted = [z_up3, z_down3, far, x_peer, z_up_x, z_down_x, z_up, z_down, xl_peer, xx_peer, right, left, partner]
    for other in greeted:
        pl.semaphore_signal(barrier, inc=1, device_id=other, device_id_type=MESH)
    scalars = [
        pltpu.make_async_copy(seeds_in, seeds, in_sem.at[YS]),
        pltpu.make_async_copy(offsets_in, offsets, in_sem.at[YS + 1]),
    ]
    for load in scalars:
        load.start()
    chunk = rows_dev // YS
    order = [y_far, y_right, y_left, y]
    loads = []
    for i, d in enumerate(order):
        where = pl.ds(pl.multiple_of(d * chunk, chunk), chunk)
        load = pltpu.make_async_copy(record.at[:, where, :], rec.at[:, where, :], in_sem.at[i])
        load.start()
        loads.append(load)


    run = chunk // STREAMS // 2

    def rows_of(d, s, half=None):
        if half is None:
            return pl.ds(pl.multiple_of(d * chunk + s * 2 * run, run), 2 * run)
        return pl.ds(pl.multiple_of(d * chunk + (s * 2 + half) * run, run), run)

    sent = [0, 0, 0]

    def send(group, src, dst, rsem, to):
        sent[group] += math.prod(src.shape) * 4
        copy = pltpu.make_async_remote_copy(
            src, dst, out_sem.at[group], rsem, device_id=to, device_id_type=MESH
        )
        copy.start()
        return copy

    def arrive(like, rsem):
        pltpu.make_async_copy(like, like, rsem).wait()

    lanes = iota((64, 128), 1)
    subs = iota((64, 128), 0)
    pattern_o = subs * C_A + lanes * C_B
    pattern_x = subs * C_B + lanes * C_A
    blocks = 2
    row0 = rw * rows_dev
    n_chunks = rows_dev // KC

    def together(matrix, vector):
        done = 0
        for i, piece in enumerate(matrix):
            piece()
            until = (i + 1) * len(vector) // len(matrix)
            for other in vector[done:until]:
                other()
            done = until

    def run_all(pieces):
        for piece in pieces:
            piece()

    def omega_hash(k):
        col0 = offsets[k] + tm * cols_dev

        def piece(i):
            base = pattern_o + ((col0 + i) * C_A + seeds[0] * C_S)
            omega[k * cols_dev + i : k * cols_dev + i + 64, :] = gauss(base, col_factor)

        return [functools.partial(piece, i) for i in range(0, cols_dev, 64)]

    def xi_hash(k):
        col0 = offsets[k] + tm * cols_dev

        def piece(i, g):
            base = pattern_x + ((col0 + i) * C_B + seeds[3] * C_S + wrapped(g * C_A))
            xit[k * cols_dev + i : k * cols_dev + i + 64, g : g + 128] = gauss(base, col_factor)

        return [functools.partial(piece, i, g) for i in range(0, cols_dev, 64) for g in range(0, CORE, 128)]

    def make_ids():
        m = iota((CORE, 128), 0)
        mine = jnp.where(m >= HALF_PHI, 1, 0)
        m = m - mine * HALF_PHI
        owner_core = jnp.where(mine == 1, c, 1 - c)
        at_z = (m * 2731) >> 16
        rest = m - at_z * 24
        at_x = jnp.where(rest >= 12, 1, 0)
        row = (at_x * (2 * ZS) + at_z * 2 + owner_core) * 12 + (rest - at_x * 12)
        phi_ids[...] = row * C_A + iota((CORE, 128), 1) * C_B
        m = iota((CORANGE, 128), 0)
        owner_core = jnp.where(m >= HALF_PSI, c, 1 - c)
        row = ((m & 15) >> 3) * 128 + ((m & 127) >> 4) * 16 + owner_core * 8 + (m & 7)
        psi_ids[...] = row * C_A + iota((CORANGE, 128), 1) * C_B

    def row_hash(kc, ids, lhs, seed):
        def piece(g, r):
            shift = (row0 + (kc * KC + g)) * C_B + seed * C_S
            lhs[r : r + 64, g : g + 128] = gauss(ids[r : r + 64, :] + shift, row_factor)

        return [functools.partial(piece, g, r) for g in range(0, KC, 128) for r in range(0, ids.shape[0], 64)]

    def phi_hash(kc):
        return row_hash(kc, phi_ids, (phi_lhs0, phi_lhs1)[kc % 2], seeds[2])

    def psi_hash(kc):
        return row_hash(kc, psi_ids, psi_lhs.at[:, kc * KC : (kc + 1) * KC], seeds[1])

    def phi_dot(kc):
        def piece(k, n):
            got = jnp.dot(
                (phi_lhs0, phi_lhs1)[kc % 2][...],
                rec[k, kc * KC : (kc + 1) * KC, n : n + 256],
                preferred_element_type=jnp.float32,
            )
            at = slice(k * cols_dev + n, k * cols_dev + n + 256)
            proj[:, at] = got if kc == 0 else proj[:, at] + got

        return [functools.partial(piece, k, n) for k in range(blocks) for n in range(0, cols_dev, 256)]

    def psi_dot(k):
        def piece(n):
            cor[:, k * cols_dev + n : k * cols_dev + n + 256] = jnp.dot(
                psi_lhs[...], rec[k, :, n : n + 256], preferred_element_type=jnp.float32
            )

        return [functools.partial(piece, n) for n in range(0, cols_dev, 256)]

    def core_dot(r0):
        def piece():
            part_of = proj[r0 : r0 + HALF_PHI, :]
            high = part_of.astype(jnp.bfloat16)
            low = (part_of - high.astype(jnp.float32)).astype(jnp.bfloat16)
            got = jnp.dot(
                jnp.concatenate([high, low], axis=0), xit[...], preferred_element_type=jnp.float32
            )
            core[r0 : r0 + HALF_PHI, :] = got[0:HALF_PHI] + got[HALF_PHI : 2 * HALF_PHI]

        return [piece]

    def range_dot(d):
        def piece(i):
            where = pl.ds(pl.multiple_of(d * chunk + i, 256), 256)
            part[where, :] = jnp.dot(
                rec[0, where, :], omega[0:cols_dev, :], preferred_element_type=jnp.float32
            ) + jnp.dot(
                rec[1, where, :], omega[cols_dev : 2 * cols_dev, :], preferred_element_type=jnp.float32
            )

        return [functools.partial(piece, i) for i in range(0, chunk, 256)]

    D = {}

    def range_forward(s):
        arrive(rb1.at[s], s1r.at[s])
        fwd[s, 0] = part[rows_of(y_right, s, 0), :] + rb1[s, 0]
        send(0, fwd.at[s, 0], rb2.at[s, 2], cr.at[s], right)
        fwd[s, 1] = part[rows_of(y_left, s, 1), :] + rb1[s, 1]
        send(0, fwd.at[s, 1], rb2.at[s, 3], cr.at[s], left)

    def range_cross(s):
        if s == 0:
            arrive(rb0, cr.at[0])
            ysum[0] = part[rows_of(y, 0), :] + rb0[0] + (rb0[1] + rb0[2])
        else:
            arrive(rb2.at[s], cr.at[s])
            ysum[s, 0:run] = part[rows_of(y, s, 0), :] + rb2[s, 2] + rb2[s, 1]
            ysum[s, run : 2 * run] = part[rows_of(y, s, 1), :] + rb2[s, 0] + rb2[s, 3]
        send(0, ysum.at[s], xb.at[s], xr.at[s], x_peer)

    def range_spread(s):
        arrive(xb.at[s], xr.at[s])
        own = rows_of(y, s)
        range_out[own, :] = ysum[s] + xb[s]
        last = s == STREAMS - 1
        if last:
            send(0, range_out.at[own], range_out.at[own], g2r.at[0], far)
        sem = g2r.at[0] if last else g1r.at[s]
        send(0, range_out.at[own], range_out.at[own], sem, right)
        send(0, range_out.at[own], range_out.at[own], sem, left)

    def range_relay(s):
        arrive(range_out.at[0 : 4 * run], g1r.at[s])
        a = rows_of(y_left, s, 0)
        send(0, range_out.at[a], range_out.at[a], g2r.at[0], right)
        b = rows_of(y_right, s, 1)
        send(0, range_out.at[b], range_out.at[b], g2r.at[0], left)

    def range_end():
        arrive(range_out.at[0 : (2 * (STREAMS - 1) + 6) * run], g2r.at[0])

    def cor_of(d, b, row, rows):
        cols = slice(b * cols_dev, (b + 1) * cols_dev)
        at = pl.ds(pl.multiple_of(d * 16 + row, 8), rows)
        mine = pl.ds(pl.multiple_of(HALF_PSI + d * 16 + row, 8), rows)
        return cor[mine, cols] + got_cor[at, cols]

    def cor_step(b, up, step):
        way = 0 if up else 1
        total = cor_of(lax.rem(z + (5 - step) if up else z + ZS - 5 + step, ZS), b, 0, 16)
        if step > (1 if b == way else 2):
            arrive(zr_cor.at[b, way, step - 2], zr.at[b, way, step - 2])
            total = total + zr_cor[b, way, step - 2]
        zs_cor[b, way, step - 1] = total
        if step < 4:
            send(
                1, zs_cor.at[b, way, step - 1], zr_cor.at[b, way, step - 1], zr.at[b, way, step - 1],
                z_up if up else z_down,
            )
        else:
            for other, to in ((0, z_up if up else z_down), (1, z_up_x if up else z_down_x)):
                row = xl * 8 if other == 0 else (1 - xl) * 8
                rows = pl.ds(pl.multiple_of(row, 8), 8)
                send(1, zs_cor.at[b, way, 3, rows], fin.at[b, 2 * way + other], fr.at[b], to)

    def cor_other(b):
        zs_own[b] = cor_of(z, b, (1 - xl) * 8, 8)
        send(1, zs_own.at[b], fin.at[b, 4], fr.at[b], xl_peer)

    def cor_final(b):
        arrive(fin.at[b], fr.at[b])
        corange_out[b] = (
            cor_of(z, b, xl * 8, 8) + fin[b, 4] + (fin[b, 0] + fin[b, 1]) + (fin[b, 2] + fin[b, 3])
        )

    def core_own(d):
        at = pl.ds(pl.multiple_of(d * 24, 8), 24)
        mine = pl.ds(pl.multiple_of(HALF_PHI + d * 24, 8), 24)
        return core[mine, :] + got_core[at, :]

    def core_gather(up):
        way = 0 if up else 1
        rows = slice(0, 16) if up else slice(16, 24)
        to = z_up if up else z_down
        zs_core[way, 0] = core_own(lax.rem(z + 4, ZS))
        zs_core[way, 1] = core_own(lax.rem(z + (2 if up else ZS - 2), ZS))
        send(1, zs_core.at[way, 0, rows], zr_core.at[way, 0, rows], kr.at[way], to)
        send(1, zs_core.at[way, 1], zr_core.at[way, 1], kr.at[way], to)

    def core_deliver(up):
        way = 0 if up else 1
        rows = slice(0, 16) if up else slice(16, 24)
        arrive(core.at[0 : 40 if up else 32], kr.at[way])
        zs_core[way, 2] = core_own(lax.rem(z + (3 if up else ZS - 3), ZS))
        zs_core[way, 2, rows, :] += zr_core[way, 0, rows, :]
        zs_core[way, 3] = core_own(lax.rem(z + (1 if up else ZS - 1), ZS)) + zr_core[way, 1]
        send(1, zs_core.at[way, 2], zr_core.at[way, 2], kr.at[2], z_up3 if up else z_down3)
        send(1, zs_core.at[way, 3], zr_core.at[way, 3], kr.at[2], z_up if up else z_down)

    def pair(what, src, dst):
        D[what] = send(2, src, dst, dr.at[what], partner)

    make_ids()
    for load in scalars:
        load.wait()
    xi = xi_hash(0) + xi_hash(1)
    run_all(omega_hash(0) + omega_hash(1) + xi[0:2])
    loads[0].wait()
    together(range_dot(y_far), xi[2:16])
    run_all(xi[16:32])
    pl.semaphore_wait(barrier, len(greeted))
    send(0, part.at[rows_of(y_far, 0)], rb0.at[0], cr.at[0], far)
    for s in range(1, STREAMS):
        send(0, part.at[rows_of(y_far, s, 0)], rb1.at[s, 0], s1r.at[s], right)
        send(0, part.at[rows_of(y_far, s, 1)], rb1.at[s, 1], s1r.at[s], left)
    for load in loads[1:]:
        load.wait()
    together(range_dot(y_right) + range_dot(y_left), xi[32:] + phi_hash(0))
    send(0, part.at[rows_of(y_right, 0)], rb0.at[1], cr.at[0], right)
    send(0, part.at[rows_of(y_left, 0)], rb0.at[2], cr.at[0], left)
    for s in range(1, STREAMS):
        send(0, part.at[rows_of(y_right, s, 1)], rb2.at[s, 0], cr.at[s], right)
        send(0, part.at[rows_of(y_left, s, 0)], rb2.at[s, 1], cr.at[s], left)
    run_all(phi_hash(1) + phi_dot(0) + phi_hash(2) + phi_dot(1) + phi_hash(3) + phi_dot(2) + psi_hash(0)[0:8] + phi_dot(3) + psi_hash(0)[8:] + core_dot(0))
    pair(2, core.at[0:HALF_PHI], got_core)
    run_all(psi_hash(1) + core_dot(HALF_PHI))
    range_forward(1)
    run_all(psi_hash(2) + range_dot(y))
    D[2].wait_recv()
    core_gather(True)
    core_gather(False)
    run_all(psi_hash(3))
    range_forward(2)
    range_forward(3)
    run_all(psi_dot(0))
    pair(0, cor.at[0:HALF_PSI, 0:cols_dev], got_cor.at[:, 0:cols_dev])
    run_all(psi_dot(1))
    pair(1, cor.at[0:HALF_PSI, cols_dev : 2 * cols_dev], got_cor.at[:, cols_dev : 2 * cols_dev])
    range_cross(0)
    D[0].wait_recv()
    cor_step(0, True, 1)
    cor_step(0, False, 2)
    cor_other(0)
    range_cross(1)
    D[1].wait_recv()
    cor_step(1, True, 2)
    cor_step(1, False, 1)
    cor_other(1)
    range_cross(2)
    core_deliver(True)
    core_deliver(False)
    range_cross(3)
    range_spread(0)
    for b, up, step in ((0, True, 2), (0, False, 3), (1, False, 2), (1, True, 3)):
        cor_step(b, up, step)
    range_spread(1)
    arrive(zr_core.at[0:2, 2:4], kr.at[2])
    both = core_own(z) + (zr_core[0, 2] + zr_core[0, 3]) + (zr_core[1, 2] + zr_core[1, 3])
    pad = jnp.zeros((4, CORE), jnp.float32)
    for i in range(2):
        shares[i, 0:12, :] = both[i * 12 : i * 12 + 12, :]
        shares[i, 12:16, :] = pad
    me_x = xh * 2 + xl
    send(2, shares.at[xl], xg.at[me_x], tr.at[0], x_peer)
    send(2, shares.at[1 - xl], xg.at[me_x], tr.at[0], xl_peer)
    send(2, shares.at[1 - xl], xg.at[me_x], tr.at[0], xx_peer)
    xg[me_x] = shares[xl]
    range_spread(2)
    for b, up, step in ((0, True, 3), (0, False, 4), (1, False, 3), (1, True, 4)):
        cor_step(b, up, step)
    range_relay(0)
    range_spread(3)
    arrive(xg.at[0:3], tr.at[0])
    yg[y] = (xg[0] + xg[1]) + (xg[2] + xg[3])
    for to in (far, right, left):
        send(2, yg.at[y], yg.at[y], ur.at[0], to)
    range_relay(1)
    cor_step(0, True, 4)
    cor_step(1, False, 4)
    range_relay(2)
    arrive(yg.at[0:3], ur.at[0])
    total = (yg[0] + yg[1]) + (yg[2] + yg[3])
    core_out[...] = total[0:12, :]
    cor_final(0)
    cor_final(1)
    range_end()
    for group, ref in enumerate((rec, part, rec)):
        rows = sent[group] // (ref.shape[-1] * ref.dtype.itemsize)
        view = ref.at[0, 0:rows] if ref is rec else ref.at[0:rows]
        arrive(view, out_sem.at[group])


def put_out(*refs):
    copies = [pltpu.make_async_copy(refs[i], refs[3 + i], refs[6].at[i]) for i in range(3)]
    for copy in copies:
        copy.start()
    for copy in copies:
        copy.wait()


def shards(record, seed_list, block_offsets):
    blocks, rows_dev, cols_dev = record.shape
    rows_count, time_count = lax.axis_size("rows"), lax.axis_size("tm")
    row_factor = 1.0 / (147.8 * math.sqrt(rows_dev * rows_count))
    col_factor = 1.0 / (147.8 * math.sqrt(blocks * cols_dev * time_count))
    run = rows_dev // YS // STREAMS // 2
    f32, bf16 = jnp.float32, jnp.bfloat16
    vmem, dma = pltpu.VMEM, pltpu.SemaphoreType.DMA
    shapes = (
        (rows_dev, RANGE),
        (blocks, CORANGE // rows_count, cols_dev),
        (CORE // rows_count, CORE),
    )
    held = pl.pallas_call(
        functools.partial(kernel, row_factor, col_factor, rows_dev, cols_dev),
        out_shape=tuple(pltpu.VMEM(shape, f32) for shape in shapes),
        in_specs=[
            pl.BlockSpec(memory_space=pl.ANY),
            pl.BlockSpec(memory_space=pl.ANY),
            pl.BlockSpec(memory_space=pl.ANY),
        ],
        out_specs=(pl.BlockSpec(memory_space=pltpu.VMEM),) * 3,
        scratch_shapes=[
            pltpu.SMEM((4,), jnp.int32),
            pltpu.SMEM((blocks,), jnp.int32),
            vmem((blocks, rows_dev, cols_dev), bf16),
            vmem((blocks * cols_dev, RANGE), bf16),
            vmem((blocks * cols_dev, CORE), bf16),
            vmem((CORE, 128), jnp.int32),
            vmem((CORANGE, 128), jnp.int32),
            vmem((CORE, KC), bf16),
            vmem((CORE, KC), bf16),
            vmem((CORANGE, rows_dev), bf16),
            vmem((CORE, blocks * cols_dev), f32),
            vmem((CORANGE, blocks * cols_dev), f32),
            vmem((CORE, CORE), f32),
            vmem((rows_dev, RANGE), f32),
            vmem((3, 2 * run, RANGE), f32),
            vmem((STREAMS, 2, run, RANGE), f32),
            vmem((STREAMS, 4, run, RANGE), f32),
            vmem((STREAMS, 2, run, RANGE), f32),
            vmem((STREAMS, 2 * run, RANGE), f32),
            vmem((STREAMS, 2 * run, RANGE), f32),
            vmem((HALF_PSI, blocks * cols_dev), f32),
            vmem((HALF_PHI, CORE), f32),
            vmem((blocks, 2, 3, 16, cols_dev), f32),
            vmem((2, 4, 24, CORE), f32),
            vmem((blocks, 2, 4, 16, cols_dev), f32),
            vmem((2, 4, 24, CORE), f32),
            vmem((blocks, 8, cols_dev), f32),
            vmem((blocks, 5, 8, cols_dev), f32),
            vmem((2, 16, CORE), f32),
            vmem((4, 16, CORE), f32),
            vmem((YS, 16, CORE), f32),
            dma((YS + 2,)),
            dma((3,)),
            dma((STREAMS,)),
            dma((STREAMS,)),
            dma((STREAMS,)),
            dma((STREAMS - 1,)),
            dma((1,)),
            dma((3,)),
            dma((blocks, 2, 3)),
            dma((blocks,)),
            dma((3,)),
            dma((1,)),
            dma((1,)),
        ],
        compiler_params=pltpu.CompilerParams(collective_id=0, has_side_effects=True),
        name="three_sketch",
    )(seed_list, block_offsets, record)
    return pl.pallas_call(
        put_out,
        out_shape=tuple(jax.ShapeDtypeStruct(shape, f32) for shape in shapes),
        in_specs=[pl.BlockSpec(memory_space=pltpu.VMEM)] * 3,
        out_specs=(pl.BlockSpec(memory_space=pl.ANY),) * 3,
        scratch_shapes=[dma((3,))],
        name="put_out",
    )(*[pltpu.with_memory_space_constraint(x, pltpu.VMEM) for x in held])


def solution(mesh):
    placed = (P(None, "rows", "tm"), P(), P())
    return jax.shard_map(
        shards,
        mesh=mesh,
        in_specs=placed,
        out_specs=(P("rows", None), P(None, "rows", "tm"), P("rows", None)),
        check_vma=False,
    )
```

```python
import functools
import math

import jax
import jax.numpy as jnp
from jax import lax
from jax.experimental import pallas as pl
from jax.experimental.pallas import tpu as pltpu
from jax.sharding import PartitionSpec as P

RANGE = 128
CORANGE = 256
CORE = 384
C_A = 668265263
C_B = 374761393
C_S = 625341585
MESH = pl.DeviceIdType.MESH

YS = 4
ZS = 8
STREAMS = 4
HALF_PSI = CORANGE // 2
HALF_PHI = CORE // 2
KC = 512


def srl(values, amount):
    return lax.shift_right_logical(values, jnp.full(values.shape, amount, jnp.int32))


def gauss(base, factor):
    h = base ^ srl(base, 15)
    h = h * 739982445
    h = h ^ srl(h, 12)
    h = h * 695872825
    h = h ^ srl(h, 15)
    pairs = (h & 0x00FF00FF) + (srl(h, 8) & 0x00FF00FF)
    total = srl(pairs * 0x00010001, 16)
    return ((total - 510).astype(jnp.float32) * factor).astype(jnp.bfloat16)


def wrapped(number):
    return (number + (1 << 31)) % (1 << 32) - (1 << 31)


def iota(shape, dim):
    return lax.broadcasted_iota(jnp.int32, shape, dim)


def kernel(
    row_factor, col_factor, rows_dev, cols_dev,
    seeds_in, offsets_in, record,
    range_out, corange_out, core_out,
    seeds, offsets, rec, omega, xit, phi_ids, psi_ids, phi_lhs0, phi_lhs1, psi_lhs, proj, cor, core,
    part, rb0, rb1, rb2, fwd, ysum, xb,
    got_cor, got_core, zr_cor, zr_core, zs_cor, zs_core, zs_own, fin, shares, xg, yg,
    in_sem, out_sem, s1r, cr, xr, g1r, g2r, dr, zr, fr, kr, tr, ur,
):
    tm, rw = lax.axis_index("tm"), lax.axis_index("rows")
    xh, y = tm // YS, lax.rem(tm, YS)
    xl, z, c = rw // (2 * ZS), lax.rem(rw // 2, ZS), lax.rem(rw, 2)

    def device(xh=xh, y=y, xl=xl, z=z, c=c):
        return (xh * YS + y, xl * (2 * ZS) + z * 2 + c)

    y_right, y_left = lax.rem(y + 1, YS), lax.rem(y + YS - 1, YS)
    y_far = lax.rem(y + 2, YS)
    right, left = device(y=y_right), device(y=y_left)
    z_up_x, z_down_x = device(z=lax.rem(z + 1, ZS), xl=1 - xl), device(z=lax.rem(z + ZS - 1, ZS), xl=1 - xl)
    z_up3, z_down3 = device(z=lax.rem(z + 3, ZS)), device(z=lax.rem(z + ZS - 3, ZS))
    x_peer = device(xh=1 - xh)
    xl_peer = device(xl=1 - xl)
    partner = device(c=1 - c)
    z_up, z_down = device(z=lax.rem(z + 1, ZS)), device(z=lax.rem(z + ZS - 1, ZS))
    far = device(y=y_far)
    xx_peer = device(xh=1 - xh, xl=1 - xl)

    barrier = pltpu.get_barrier_semaphore()
    greeted = [z_up3, z_down3, far, x_peer, z_up_x, z_down_x, z_up, z_down, xl_peer, xx_peer, right, left, partner]
    for other in greeted:
        pl.semaphore_signal(barrier, inc=1, device_id=other, device_id_type=MESH)
    scalars = [
        pltpu.make_async_copy(seeds_in, seeds, in_sem.at[YS]),
        pltpu.make_async_copy(offsets_in, offsets, in_sem.at[YS + 1]),
    ]
    for load in scalars:
        load.start()
    chunk = rows_dev // YS
    order = [y_far, y_right, y_left, y]
    loads = []
    for i, d in enumerate(order):
        where = pl.ds(pl.multiple_of(d * chunk, chunk), chunk)
        load = pltpu.make_async_copy(record.at[:, where, :], rec.at[:, where, :], in_sem.at[i])
        load.start()
        loads.append(load)


    run = chunk // STREAMS // 2

    def rows_of(d, s, half=None):
        if half is None:
            return pl.ds(pl.multiple_of(d * chunk + s * 2 * run, run), 2 * run)
        return pl.ds(pl.multiple_of(d * chunk + (s * 2 + half) * run, run), run)

    sent = [0, 0, 0]

    def send(group, src, dst, rsem, to):
        sent[group] += math.prod(src.shape) * 4
        copy = pltpu.make_async_remote_copy(
            src, dst, out_sem.at[group], rsem, device_id=to, device_id_type=MESH
        )
        copy.start()
        return copy

    def arrive(like, rsem):
        pltpu.make_async_copy(like, like, rsem).wait()

    lanes = iota((64, 128), 1)
    subs = iota((64, 128), 0)
    pattern_o = subs * C_A + lanes * C_B
    pattern_x = subs * C_B + lanes * C_A
    blocks = 2
    row0 = rw * rows_dev
    n_chunks = rows_dev // KC

    def together(matrix, vector):
        done = 0
        for i, piece in enumerate(matrix):
            piece()
            until = (i + 1) * len(vector) // len(matrix)
            for other in vector[done:until]:
                other()
            done = until

    def run_all(pieces):
        for piece in pieces:
            piece()

    def omega_hash(k):
        col0 = offsets[k] + tm * cols_dev

        def piece(i):
            base = pattern_o + ((col0 + i) * C_A + seeds[0] * C_S)
            omega[k * cols_dev + i : k * cols_dev + i + 64, :] = gauss(base, col_factor)

        return [functools.partial(piece, i) for i in range(0, cols_dev, 64)]

    def xi_hash(k):
        col0 = offsets[k] + tm * cols_dev

        def piece(i, g):
            base = pattern_x + ((col0 + i) * C_B + seeds[3] * C_S + wrapped(g * C_A))
            xit[k * cols_dev + i : k * cols_dev + i + 64, g : g + 128] = gauss(base, col_factor)

        return [functools.partial(piece, i, g) for i in range(0, cols_dev, 64) for g in range(0, CORE, 128)]

    def make_ids():
        m = iota((CORE, 128), 0)
        mine = jnp.where(m >= HALF_PHI, 1, 0)
        m = m - mine * HALF_PHI
        owner_core = jnp.where(mine == 1, c, 1 - c)
        at_z = (m * 2731) >> 16
        rest = m - at_z * 24
        at_x = jnp.where(rest >= 12, 1, 0)
        row = (at_x * (2 * ZS) + at_z * 2 + owner_core) * 12 + (rest - at_x * 12)
        phi_ids[...] = row * C_A + iota((CORE, 128), 1) * C_B
        m = iota((CORANGE, 128), 0)
        owner_core = jnp.where(m >= HALF_PSI, c, 1 - c)
        row = ((m & 15) >> 3) * 128 + ((m & 127) >> 4) * 16 + owner_core * 8 + (m & 7)
        psi_ids[...] = row * C_A + iota((CORANGE, 128), 1) * C_B

    def row_hash(kc, ids, lhs, seed):
        def piece(g, r):
            shift = (row0 + (kc * KC + g)) * C_B + seed * C_S
            lhs[r : r + 64, g : g + 128] = gauss(ids[r : r + 64, :] + shift, row_factor)

        return [functools.partial(piece, g, r) for g in range(0, KC, 128) for r in range(0, ids.shape[0], 64)]

    def phi_hash(kc):
        return row_hash(kc, phi_ids, (phi_lhs0, phi_lhs1)[kc % 2], seeds[2])

    def psi_hash(kc):
        return row_hash(kc, psi_ids, psi_lhs.at[:, kc * KC : (kc + 1) * KC], seeds[1])

    def phi_dot(kc):
        def piece(k, n):
            got = jnp.dot(
                (phi_lhs0, phi_lhs1)[kc % 2][...],
                rec[k, kc * KC : (kc + 1) * KC, n : n + 256],
                preferred_element_type=jnp.float32,
            )
            at = slice(k * cols_dev + n, k * cols_dev + n + 256)
            proj[:, at] = got if kc == 0 else proj[:, at] + got

        return [functools.partial(piece, k, n) for k in range(blocks) for n in range(0, cols_dev, 256)]

    def psi_dot(k):
        def piece(n):
            cor[:, k * cols_dev + n : k * cols_dev + n + 256] = jnp.dot(
                psi_lhs[...], rec[k, :, n : n + 256], preferred_element_type=jnp.float32
            )

        return [functools.partial(piece, n) for n in range(0, cols_dev, 256)]

    def core_dot(r0):
        def piece():
            part_of = proj[r0 : r0 + HALF_PHI, :]
            high = part_of.astype(jnp.bfloat16)
            low = (part_of - high.astype(jnp.float32)).astype(jnp.bfloat16)
            got = jnp.dot(
                jnp.concatenate([high, low], axis=0), xit[...], preferred_element_type=jnp.float32
            )
            core[r0 : r0 + HALF_PHI, :] = got[0:HALF_PHI] + got[HALF_PHI : 2 * HALF_PHI]

        return [piece]

    def range_dot(d):
        def piece(i):
            where = pl.ds(pl.multiple_of(d * chunk + i, 256), 256)
            part[where, :] = jnp.dot(
                rec[0, where, :], omega[0:cols_dev, :], preferred_element_type=jnp.float32
            ) + jnp.dot(
                rec[1, where, :], omega[cols_dev : 2 * cols_dev, :], preferred_element_type=jnp.float32
            )

        return [functools.partial(piece, i) for i in range(0, chunk, 256)]

    D = {}

    def range_forward(s):
        arrive(rb1.at[s], s1r.at[s])
        fwd[s, 0] = part[rows_of(y_right, s, 0), :] + rb1[s, 0]
        send(0, fwd.at[s, 0], rb2.at[s, 2], cr.at[s], right)
        fwd[s, 1] = part[rows_of(y_left, s, 1), :] + rb1[s, 1]
        send(0, fwd.at[s, 1], rb2.at[s, 3], cr.at[s], left)

    def range_cross(s):
        if s == 0:
            arrive(rb0, cr.at[0])
            ysum[0] = part[rows_of(y, 0), :] + rb0[0] + (rb0[1] + rb0[2])
        else:
            arrive(rb2.at[s], cr.at[s])
            ysum[s, 0:run] = part[rows_of(y, s, 0), :] + rb2[s, 2] + rb2[s, 1]
            ysum[s, run : 2 * run] = part[rows_of(y, s, 1), :] + rb2[s, 0] + rb2[s, 3]
        send(0, ysum.at[s], xb.at[s], xr.at[s], x_peer)

    def range_spread(s):
        arrive(xb.at[s], xr.at[s])
        own = rows_of(y, s)
        range_out[own, :] = ysum[s] + xb[s]
        last = s == STREAMS - 1
        if last:
            send(0, range_out.at[own], range_out.at[own], g2r.at[0], far)
        sem = g2r.at[0] if last else g1r.at[s]
        send(0, range_out.at[own], range_out.at[own], sem, right)
        send(0, range_out.at[own], range_out.at[own], sem, left)

    def range_relay(s):
        arrive(range_out.at[0 : 4 * run], g1r.at[s])
        a = rows_of(y_left, s, 0)
        send(0, range_out.at[a], range_out.at[a], g2r.at[0], right)
        b = rows_of(y_right, s, 1)
        send(0, range_out.at[b], range_out.at[b], g2r.at[0], left)

    def range_end():
        arrive(range_out.at[0 : (2 * (STREAMS - 1) + 6) * run], g2r.at[0])

    def cor_of(d, b, row, rows):
        cols = slice(b * cols_dev, (b + 1) * cols_dev)
        at = pl.ds(pl.multiple_of(d * 16 + row, 8), rows)
        mine = pl.ds(pl.multiple_of(HALF_PSI + d * 16 + row, 8), rows)
        return cor[mine, cols] + got_cor[at, cols]

    def cor_step(b, up, step):
        way = 0 if up else 1
        total = cor_of(lax.rem(z + (5 - step) if up else z + ZS - 5 + step, ZS), b, 0, 16)
        if step > (1 if b == way else 2):
            arrive(zr_cor.at[b, way, step - 2], zr.at[b, way, step - 2])
            total = total + zr_cor[b, way, step - 2]
        zs_cor[b, way, step - 1] = total
        if step < 4:
            send(
                1, zs_cor.at[b, way, step - 1], zr_cor.at[b, way, step - 1], zr.at[b, way, step - 1],
                z_up if up else z_down,
            )
        else:
            for other, to in ((0, z_up if up else z_down), (1, z_up_x if up else z_down_x)):
                row = xl * 8 if other == 0 else (1 - xl) * 8
                rows = pl.ds(pl.multiple_of(row, 8), 8)
                send(1, zs_cor.at[b, way, 3, rows], fin.at[b, 2 * way + other], fr.at[b], to)

    def cor_other(b):
        zs_own[b] = cor_of(z, b, (1 - xl) * 8, 8)
        send(1, zs_own.at[b], fin.at[b, 4], fr.at[b], xl_peer)

    def cor_final(b):
        arrive(fin.at[b], fr.at[b])
        corange_out[b] = (
            cor_of(z, b, xl * 8, 8) + fin[b, 4] + (fin[b, 0] + fin[b, 1]) + (fin[b, 2] + fin[b, 3])
        )

    def core_own(d):
        at = pl.ds(pl.multiple_of(d * 24, 8), 24)
        mine = pl.ds(pl.multiple_of(HALF_PHI + d * 24, 8), 24)
        return core[mine, :] + got_core[at, :]

    def core_gather(up):
        way = 0 if up else 1
        rows = slice(0, 16) if up else slice(16, 24)
        to = z_up if up else z_down
        zs_core[way, 0] = core_own(lax.rem(z + 4, ZS))
        zs_core[way, 1] = core_own(lax.rem(z + (2 if up else ZS - 2), ZS))
        send(1, zs_core.at[way, 0, rows], zr_core.at[way, 0, rows], kr.at[way], to)
        send(1, zs_core.at[way, 1], zr_core.at[way, 1], kr.at[way], to)

    def core_deliver(up):
        way = 0 if up else 1
        rows = slice(0, 16) if up else slice(16, 24)
        arrive(core.at[0 : 40 if up else 32], kr.at[way])
        zs_core[way, 2] = core_own(lax.rem(z + (3 if up else ZS - 3), ZS))
        zs_core[way, 2, rows, :] += zr_core[way, 0, rows, :]
        zs_core[way, 3] = core_own(lax.rem(z + (1 if up else ZS - 1), ZS)) + zr_core[way, 1]
        send(1, zs_core.at[way, 2], zr_core.at[way, 2], kr.at[2], z_up3 if up else z_down3)
        send(1, zs_core.at[way, 3], zr_core.at[way, 3], kr.at[2], z_up if up else z_down)

    def pair(what, src, dst):
        D[what] = send(2, src, dst, dr.at[what], partner)

    make_ids()
    for load in scalars:
        load.wait()
    xi = xi_hash(0) + xi_hash(1)
    run_all(omega_hash(0) + omega_hash(1) + xi[0:2])
    loads[0].wait()
    together(range_dot(y_far), xi[2:16])
    run_all(xi[16:32])
    pl.semaphore_wait(barrier, len(greeted))
    send(0, part.at[rows_of(y_far, 0)], rb0.at[0], cr.at[0], far)
    for s in range(1, STREAMS):
        send(0, part.at[rows_of(y_far, s, 0)], rb1.at[s, 0], s1r.at[s], right)
        send(0, part.at[rows_of(y_far, s, 1)], rb1.at[s, 1], s1r.at[s], left)
    for load in loads[1:]:
        load.wait()
    together(range_dot(y_right) + range_dot(y_left), xi[32:] + phi_hash(0))
    send(0, part.at[rows_of(y_right, 0)], rb0.at[1], cr.at[0], right)
    send(0, part.at[rows_of(y_left, 0)], rb0.at[2], cr.at[0], left)
    for s in range(1, STREAMS):
        send(0, part.at[rows_of(y_right, s, 1)], rb2.at[s, 0], cr.at[s], right)
        send(0, part.at[rows_of(y_left, s, 0)], rb2.at[s, 1], cr.at[s], left)
    run_all(phi_hash(1) + phi_dot(0) + phi_hash(2) + phi_dot(1) + phi_hash(3) + phi_dot(2) + psi_hash(0)[0:8] + phi_dot(3) + psi_hash(0)[8:] + core_dot(0))
    pair(2, core.at[0:HALF_PHI], got_core)
    run_all(psi_hash(1) + core_dot(HALF_PHI))
    range_forward(1)
    run_all(psi_hash(2) + range_dot(y))
    D[2].wait_recv()
    core_gather(True)
    core_gather(False)
    run_all(psi_hash(3))
    range_forward(2)
    range_forward(3)
    run_all(psi_dot(0))
    pair(0, cor.at[0:HALF_PSI, 0:cols_dev], got_cor.at[:, 0:cols_dev])
    run_all(psi_dot(1))
    pair(1, cor.at[0:HALF_PSI, cols_dev : 2 * cols_dev], got_cor.at[:, cols_dev : 2 * cols_dev])
    range_cross(0)
    D[0].wait_recv()
    cor_step(0, True, 1)
    cor_step(0, False, 2)
    cor_other(0)
    D[1].wait_recv()
    cor_step(1, True, 2)
    cor_step(1, False, 1)
    cor_other(1)
    core_deliver(True)
    core_deliver(False)
    range_cross(1)
    range_cross(2)
    range_cross(3)
    range_spread(0)
    for b, up, step in ((0, True, 2), (0, False, 3), (1, False, 2), (1, True, 3)):
        cor_step(b, up, step)
    range_spread(1)
    arrive(zr_core.at[0:2, 2:4], kr.at[2])
    both = core_own(z) + (zr_core[0, 2] + zr_core[0, 3]) + (zr_core[1, 2] + zr_core[1, 3])
    pad = jnp.zeros((4, CORE), jnp.float32)
    for i in range(2):
        shares[i, 0:12, :] = both[i * 12 : i * 12 + 12, :]
        shares[i, 12:16, :] = pad
    me_x = xh * 2 + xl
    send(2, shares.at[xl], xg.at[me_x], tr.at[0], x_peer)
    send(2, shares.at[1 - xl], xg.at[me_x], tr.at[0], xl_peer)
    send(2, shares.at[1 - xl], xg.at[me_x], tr.at[0], xx_peer)
    xg[me_x] = shares[xl]
    range_spread(2)
    for b, up, step in ((0, True, 3), (0, False, 4), (1, False, 3), (1, True, 4)):
        cor_step(b, up, step)
    range_relay(0)
    range_spread(3)
    arrive(xg.at[0:3], tr.at[0])
    yg[y] = (xg[0] + xg[1]) + (xg[2] + xg[3])
    for to in (far, right, left):
        send(2, yg.at[y], yg.at[y], ur.at[0], to)
    range_relay(1)
    cor_step(0, True, 4)
    cor_step(1, False, 4)
    range_relay(2)
    arrive(yg.at[0:3], ur.at[0])
    total = (yg[0] + yg[1]) + (yg[2] + yg[3])
    core_out[...] = total[0:12, :]
    cor_final(0)
    cor_final(1)
    range_end()
    for group, ref in enumerate((rec, part, rec)):
        rows = sent[group] // (ref.shape[-1] * ref.dtype.itemsize)
        view = ref.at[0, 0:rows] if ref is rec else ref.at[0:rows]
        arrive(view, out_sem.at[group])


def put_out(*refs):
    copies = [pltpu.make_async_copy(refs[i], refs[3 + i], refs[6].at[i]) for i in range(3)]
    for copy in copies:
        copy.start()
    for copy in copies:
        copy.wait()


def shards(record, seed_list, block_offsets):
    blocks, rows_dev, cols_dev = record.shape
    rows_count, time_count = lax.axis_size("rows"), lax.axis_size("tm")
    row_factor = 1.0 / (147.8 * math.sqrt(rows_dev * rows_count))
    col_factor = 1.0 / (147.8 * math.sqrt(blocks * cols_dev * time_count))
    run = rows_dev // YS // STREAMS // 2
    f32, bf16 = jnp.float32, jnp.bfloat16
    vmem, dma = pltpu.VMEM, pltpu.SemaphoreType.DMA
    shapes = (
        (rows_dev, RANGE),
        (blocks, CORANGE // rows_count, cols_dev),
        (CORE // rows_count, CORE),
    )
    held = pl.pallas_call(
        functools.partial(kernel, row_factor, col_factor, rows_dev, cols_dev),
        out_shape=tuple(pltpu.VMEM(shape, f32) for shape in shapes),
        in_specs=[
            pl.BlockSpec(memory_space=pl.ANY),
            pl.BlockSpec(memory_space=pl.ANY),
            pl.BlockSpec(memory_space=pl.ANY),
        ],
        out_specs=(pl.BlockSpec(memory_space=pltpu.VMEM),) * 3,
        scratch_shapes=[
            pltpu.SMEM((4,), jnp.int32),
            pltpu.SMEM((blocks,), jnp.int32),
            vmem((blocks, rows_dev, cols_dev), bf16),
            vmem((blocks * cols_dev, RANGE), bf16),
            vmem((blocks * cols_dev, CORE), bf16),
            vmem((CORE, 128), jnp.int32),
            vmem((CORANGE, 128), jnp.int32),
            vmem((CORE, KC), bf16),
            vmem((CORE, KC), bf16),
            vmem((CORANGE, rows_dev), bf16),
            vmem((CORE, blocks * cols_dev), f32),
            vmem((CORANGE, blocks * cols_dev), f32),
            vmem((CORE, CORE), f32),
            vmem((rows_dev, RANGE), f32),
            vmem((3, 2 * run, RANGE), f32),
            vmem((STREAMS, 2, run, RANGE), f32),
            vmem((STREAMS, 4, run, RANGE), f32),
            vmem((STREAMS, 2, run, RANGE), f32),
            vmem((STREAMS, 2 * run, RANGE), f32),
            vmem((STREAMS, 2 * run, RANGE), f32),
            vmem((HALF_PSI, blocks * cols_dev), f32),
            vmem((HALF_PHI, CORE), f32),
            vmem((blocks, 2, 3, 16, cols_dev), f32),
            vmem((2, 4, 24, CORE), f32),
            vmem((blocks, 2, 4, 16, cols_dev), f32),
            vmem((2, 4, 24, CORE), f32),
            vmem((blocks, 8, cols_dev), f32),
            vmem((blocks, 5, 8, cols_dev), f32),
            vmem((2, 16, CORE), f32),
            vmem((4, 16, CORE), f32),
            vmem((YS, 16, CORE), f32),
            dma((YS + 2,)),
            dma((3,)),
            dma((STREAMS,)),
            dma((STREAMS,)),
            dma((STREAMS,)),
            dma((STREAMS - 1,)),
            dma((1,)),
            dma((3,)),
            dma((blocks, 2, 3)),
            dma((blocks,)),
            dma((3,)),
            dma((1,)),
            dma((1,)),
        ],
        compiler_params=pltpu.CompilerParams(collective_id=0, has_side_effects=True),
        name="three_sketch",
    )(seed_list, block_offsets, record)
    return pl.pallas_call(
        put_out,
        out_shape=tuple(jax.ShapeDtypeStruct(shape, f32) for shape in shapes),
        in_specs=[pl.BlockSpec(memory_space=pltpu.VMEM)] * 3,
        out_specs=(pl.BlockSpec(memory_space=pl.ANY),) * 3,
        scratch_shapes=[dma((3,))],
        name="put_out",
    )(*[pltpu.with_memory_space_constraint(x, pltpu.VMEM) for x in held])


def solution(mesh):
    placed = (P(None, "rows", "tm"), P(), P())
    return jax.shard_map(
        shards,
        mesh=mesh,
        in_specs=placed,
        out_specs=(P("rows", None), P(None, "rows", "tm"), P("rows", None)),
        check_vma=False,
    )
```
